32 devices in a mesh: slab: 4 (over x, core), patch: 8 (over z, y).
Axes of the slice: x: 2, y: 2, z: 4, core: 2. Of those that a mesh axis runs over, the one named last changes fastest.
Arguments:
- right_side: float32 [4, 8, 256, 768], P('slab', 'patch'), may hold values from -6 to 6
- inverse_factor: bfloat16 [4, 8, 768, 768], P('slab', 'patch'), may hold values from -0.12990381 to 1.5, as said below
- forward_trace: bfloat16 [4, 8, 128, 768], P('slab', 'patch'), may hold values from -0.375 to 0.375
- backward_trace: bfloat16 [4, 8, 128, 768], P('slab', 'patch'), may hold values from -0.375 to 0.375
- margin: int32 [4, 8], P('slab', 'patch'), may hold values from 1 to 256, as said below
Outputs:
- correction: float32 [4, 8, 256, 768], P('slab', 'patch')
The draws below stay inside these ranges and needn't reach their ends.
Inputs may be any that keep to these rules, and one draw needn't show every extreme that they name: `inverse_factor`: lower triangular: zero above the diagonal, positive on it. margin[s, q] counts the last unknowns of patch q that are the first unknowns of patch q + 1 (of patch 0 for q = 7). In every slab some pair shares exactly 256.
All inputs are finite; a program needn't handle non-finite values.
Results may differ from the reference program's by a relative error of at most 0.035.
Values may be sent and summed in bfloat16 or wider, within the bound.
A program may use at most 64 MiB of HBM per device.

```python
import math
import jax
import jax.numpy as jnp
from jax import lax

M = 768
KMAX = 256
FACE = 128
COLS = 256
SLABS = 4
PATCHES = 8


def draw_inverse_factor(key, part):
    first_key = jax.random.fold_in(key, 11)
    second_key = jax.random.fold_in(key, 12)
    full_shape = (SLABS, PATCHES, M, M)
    spread = jnp.clip(0.6 * jax.random.normal(first_key, full_shape, jnp.float32), -3.6, 3.6)
    diagonal = jax.random.uniform(second_key, (SLABS, PATCHES, M), jnp.float32, 0.7, 1.3)
    row_index = jnp.arange(M)[:, None]
    col_index = jnp.arange(M)[None, :]
    lower_part = jnp.where(row_index > col_index, spread, 0.0) / math.sqrt(M)
    matrix = lower_part + jnp.where(row_index == col_index, 1.0, 0.0) * diagonal[..., :, None]
    return matrix.astype(jnp.bfloat16)


def draw_margin(key, part):
    values = jax.random.randint(jax.random.fold_in(key, 21), (SLABS, PATCHES), 1, KMAX + 1)
    chosen = jax.random.randint(jax.random.fold_in(key, 22), (SLABS, 1), 0, PATCHES)
    return jnp.where(jnp.arange(PATCHES)[None, :] == chosen, KMAX, values).astype(jnp.int32)


def steps_of(key, shape, cuts, least, largest):
    level, own = 1.0, jax.random.fold_in(key, 6)
    for axis_at, shards_of in cuts:
        draws = jnp.exp(jax.random.uniform(jax.random.fold_in(own, axis_at), (shards_of,), jnp.float32, least / len(cuts), largest / len(cuts)))
        level = level * jnp.repeat(draws, shape[axis_at] // shards_of).reshape([-1 if axis == axis_at else 1 for axis in range(len(shape))])
    return level


def gaussian(stream_key, extent, width, bound, cuts=(), kind=jnp.bfloat16):
    drawn = jax.random.normal(stream_key, extent, jnp.float32) * width
    if len(cuts) > 0:
        drawn = steps_of(stream_key, extent, cuts, -0.22, 0.18) * drawn
    return jnp.clip(drawn, min=-bound, max=bound).astype(kind)


def setup_inputs(seed: int = 0) -> dict:
    keys = jax.random.split(jax.random.key(seed), 6)
    right_side = gaussian(keys[0], (SLABS, PATCHES, COLS, M), 1.0, 6.0, ((0, 4), (1, 8)), jnp.float32)
    inverse_factor = draw_inverse_factor(jax.random.fold_in(keys[5], 71), 0)
    forward_trace = gaussian(keys[2], (SLABS, PATCHES, FACE, M), (2 * FACE) ** -0.5, 0.375, ((0, 4), (1, 8)))
    backward_trace = gaussian(keys[3], (SLABS, PATCHES, FACE, M), (2 * FACE) ** -0.5, 0.375, ((0, 4), (1, 8)))
    margin = draw_margin(jax.random.fold_in(keys[5], 71), 0)
    return {"right_side": right_side, "inverse_factor": inverse_factor, "forward_trace": forward_trace, "backward_trace": backward_trace, "margin": margin}


def to_half(values):
    return lax.optimization_barrier(values.astype(jnp.bfloat16)).astype(jnp.float32)


def placement(counts):
    source_index = jnp.arange(KMAX, dtype=jnp.int32)[None, :, None]
    target_index = jnp.arange(KMAX, dtype=jnp.int32)[None, None, :]
    limit = counts.astype(jnp.int32)[:, None, None]
    hit = (source_index == KMAX - limit + target_index) & (target_index < limit)
    return jnp.where(hit, 1.0, 0.0).astype(jnp.float32)


def solve(values, factor):
    halfway = to_half(jnp.einsum('pck,pik->pci', to_half(values), factor))
    return jnp.einsum('pci,pik->pck', halfway, factor)


def slab_step(residual, factor, counts):
    initial = to_half(solve(residual, factor))
    placing = placement(counts)
    tail_rows = initial[:, :, M - KMAX:]
    head_rows = initial[:, :, :KMAX]
    from_left = jnp.roll(jnp.einsum('pcs,psd->pcd', tail_rows, placing), 1, axis=0)
    from_right = jnp.einsum('pci,pti->pct', jnp.roll(head_rows, -1, axis=0), placing)
    middle = jnp.zeros((residual.shape[0], residual.shape[1], M - 2 * KMAX), jnp.float32)
    shared = jnp.concatenate([from_left, middle, from_right], axis=2)
    return solve(residual - 0.5 * shared, factor)


def face_map(matrix, corrected):
    return to_half(jnp.einsum('pck,ptk->pct', to_half(corrected), matrix))


def face_terms(down_face, up_face):
    middle = jnp.zeros((down_face.shape[0], down_face.shape[1], M - 2 * FACE), jnp.float32)
    return jnp.concatenate([down_face, middle, up_face], axis=2)


def reference(right_side, inverse_factor, forward_trace, backward_trace, margin):
    zero_face = jnp.zeros((PATCHES, COLS, FACE), jnp.float32)
    down_store = []
    arriving = zero_face
    forward_last = None
    for slab_index in range(SLABS):
        factor = inverse_factor[slab_index].astype(jnp.float32)
        residual = right_side[slab_index] - face_terms(arriving, zero_face)
        corrected = slab_step(residual, factor, margin[slab_index])
        down_store.append(arriving)
        arriving = face_map(forward_trace[slab_index].astype(jnp.float32), corrected)
        forward_last = corrected
    results = [None] * SLABS
    up_face = zero_face
    for slab_index in range(SLABS - 1, -1, -1):
        factor = inverse_factor[slab_index].astype(jnp.float32)
        if slab_index == SLABS - 1:
            corrected = forward_last
        else:
            residual = right_side[slab_index] - face_terms(down_store[slab_index], up_face)
            corrected = slab_step(residual, factor, margin[slab_index])
        results[slab_index] = corrected
        up_face = face_map(backward_trace[slab_index].astype(jnp.float32), corrected)
    return jnp.stack(results, axis=0)
```

```python
import functools

import jax
import jax.numpy as jnp
from jax import lax
from jax.experimental import pallas as pl
from jax.experimental.pallas import tpu as pltpu
from jax.sharding import PartitionSpec as P

KMAX = 256
BF = jnp.bfloat16
F32 = jnp.float32
MESH = pl.DeviceIdType.MESH


def nt(a, b):
    return lax.dot_general(a, b, (((1,), (1,)), ((), ())), preferred_element_type=F32)


def nn(a, b):
    return lax.dot_general(a, b, (((1,), (0,)), ((), ())), preferred_element_type=F32)


def tn(a, b):
    return lax.dot_general(a, b, (((0,), (0,)), ((), ())), preferred_element_type=F32)


def halfway(x, fac, m):
    return jnp.concatenate(
        [nt(x[:, : i + KMAX], fac[i : i + KMAX, : i + KMAX]).astype(BF) for i in range(0, m, KMAX)],
        axis=1,
    )


def solve(x, fac, m):
    half = halfway(x, fac, m)
    return [nn(half[:, k:], fac[k:, k : k + KMAX]) for k in range(0, m, KMAX)]


def finish(half_ref, l_ref, out_ref, held, sem):
    m = half_ref.shape[1]
    copies = []
    for n, k in enumerate(range(0, m, KMAX)):
        held[n] = nn(half_ref[:, k:], l_ref[0, 0, k:, k : k + KMAX])
        copies.append(pltpu.make_async_copy(held.at[n], out_ref.at[0, 0, :, k : k + KMAX], sem.at[n]))
        copies[-1].start()
    for c in copies:
        c.wait()


def kernel(
    slabs, patches, parts,
    r_hbm, l_hbm, f_hbm, b_hbm, margin_ref, out_ref,
    r_v, fac, maps,
    tail_s, head_s, zt_s, zh_s, d_s, u_s,
    tail_r, head_r, zt_r, zh_r, d_r, u_r,
    adj, acc, gt, opd, opu, place, zr,
    load_sem, send_sem, recv_sem,
):
    s = lax.axis_index("slab")
    q = lax.axis_index("patch")
    left = lax.rem(q + patches - 1, patches)
    right = lax.rem(q + 1, patches)
    around = (left, right, q)
    m = fac.shape[-1]
    face = f_hbm.shape[-2]
    cols = r_v.shape[0]
    step = cols // parts
    first_slab, last_slab = s == 0, s == slabs - 1
    inner_low, inner_high = s > 0, s < slabs - 1

    loads = [
        pltpu.make_async_copy(r_hbm.at[0, 0], r_v, load_sem.at[0]),
        pltpu.make_async_copy(l_hbm.at[0, 0], fac, load_sem.at[1]),
        pltpu.make_async_copy(f_hbm.at[0, 0], maps.at[:face], load_sem.at[2]),
        pltpu.make_async_copy(b_hbm.at[0, 0], maps.at[face:], load_sem.at[3]),
    ]
    for c in loads:
        c.start()

    barrier = pltpu.get_barrier_semaphore()

    def greet(slab, patch):
        pl.semaphore_signal(barrier, inc=1, device_id=(slab, patch), device_id_type=MESH)

    greet(s, left)
    greet(s, right)

    @pl.when(inner_low)
    def _():
        for p in around:
            greet(s - 1, p)

    @pl.when(inner_high)
    def _():
        for p in around:
            greet(s + 1, p)

    slot = [0]

    def send(src, dst, slab, patch):
        n = slot[0]
        slot[0] += 1
        return pltpu.make_async_remote_copy(
            src_ref=src, dst_ref=dst, send_sem=send_sem.at[n], recv_sem=recv_sem.at[n],
            device_id=(slab, patch), device_id_type=MESH,
        )

    rows = [pl.ds(c * step, step) for c in range(parts)]
    tail_c = [send(tail_s.at[w], tail_r.at[w], s, right) for w in rows]
    head_c = [send(head_s.at[w], head_r.at[w], s, left) for w in rows]
    low_rows, high_rows = pl.ds(0, face), pl.ds(face, face)
    zd_c = [send(zt_s.at[low_rows], zt_r.at[low_rows], s, right), send(zh_s.at[low_rows], zh_r.at[low_rows], s, left)]
    zu_c = [send(zt_s.at[high_rows], zt_r.at[high_rows], s, right), send(zh_s.at[high_rows], zh_r.at[high_rows], s, left)]
    targets = ((2, left), (1, right), (0, q))
    down_c = [[send(d_s.at[w], d_r.at[j, w], s + 1, p) for j, p in targets] for w in rows]
    up_c = [[send(u_s.at[w], u_r.at[j, w], s - 1, p) for j, p in targets] for w in rows]

    count = margin_ref[0, 0]
    row = lax.broadcasted_iota(jnp.int32, (KMAX, KMAX), 0)
    col = lax.broadcasted_iota(jnp.int32, (KMAX, KMAX), 1)
    hit = (row == KMAX - count + col) & (col < count)
    place[...] = jnp.where(hit, 1.0, 0.0).astype(BF)

    loads[0].wait()
    loads[1].wait()
    first = solve(r_v[...].astype(BF), fac, m)
    tail_s[...] = nn(first[-1].astype(BF), place[...]).astype(BF)
    head_s[...] = first[0].astype(BF)

    pl.semaphore_wait(barrier, 2 + 3 * inner_low.astype(jnp.int32) + 3 * inner_high.astype(jnp.int32))

    for a, b in zip(tail_c, head_c):
        a.start()
        b.start()

    loads[2].wait()
    loads[3].wait()
    for k, part in enumerate(solve(maps[...], fac, m)):
        gt[:, k * KMAX : (k + 1) * KMAX] = part.astype(BF)

    low = fac[:, :face]
    high = fac[m - face :, m - face :]
    k_tail = jnp.concatenate(
        [tn(low[m - KMAX :], fac[m - KMAX :, m - KMAX :]), tn(high, fac[m - face :, m - KMAX :])], axis=0
    )
    k_head = jnp.concatenate([tn(low, fac[:, :KMAX]), tn(high, fac[m - face :, :KMAX])], axis=0)
    zt_s[...] = nn(k_tail.astype(BF), place[...]).astype(BF)
    zh_s[...] = k_head.astype(BF)

    @pl.when(inner_low)
    def _():
        for c in zd_c:
            c.start()

    @pl.when(inner_low & inner_high)
    def _():
        for c in zu_c:
            c.start()

    def send_down(c):
        w = rows[c]
        d_s[w] = acc[w, :face].astype(BF)
        for x in down_c[c]:
            x.start()

    def send_up(c):
        w = rows[c]
        u_s[w] = acc[w, face:].astype(BF)
        for x in up_c[c]:
            x.start()

    for c, w in enumerate(rows):
        tail_c[c].wait_recv()
        head_c[c].wait_recv()
        adj[w, :] = r_v[w, :]
        adj[w, :KMAX] = adj[w, :KMAX] - 0.5 * tail_r[w].astype(F32)
        adj[w, m - KMAX :] = adj[w, m - KMAX :] - 0.5 * nt(head_r[w], place[...])
        acc[w, :face] = nt(adj[w, :].astype(BF), gt[:face])

        @pl.when(first_slab)
        def _():
            send_down(c)

    @pl.when(first_slab)
    def _():
        for c in zu_c:
            c.start()

    acc[:, face:] = nt(adj[...].astype(BF), gt[face:])

    @pl.when(inner_low)
    def _():
        for c in zd_c:
            c.wait_recv()
        zr[low_rows] = nt(zh_r[low_rows], place[...]).astype(BF)
        opd[:face, :] = (-gt[:, :face].astype(F32)).T.astype(BF)
        opd[face : 2 * face, :] = (0.5 * nt(zt_r[low_rows], gt[:, :KMAX])).astype(BF)
        opd[2 * face :, :] = (0.5 * nt(zr[low_rows], gt[:, m - KMAX :])).astype(BF)

    def make_up():
        for c in zu_c:
            c.wait_recv()
        zr[high_rows] = nt(zh_r[high_rows], place[...]).astype(BF)

        @pl.when(inner_low)
        def _():
            opu[:face, :] = (-gt[face:, m - face :].astype(F32)).T.astype(BF)
            opu[face : 2 * face, :] = (0.5 * nt(zt_r[high_rows], gt[face:, :KMAX])).astype(BF)
            opu[2 * face :, :] = (0.5 * nt(zr[high_rows], gt[face:, m - KMAX :])).astype(BF)

    def beside(ref, w):
        return jnp.concatenate([ref[0, w], ref[1, w], ref[2, w]], axis=1)

    @pl.when(inner_low)
    def _():
        for c, w in enumerate(rows):
            for x in down_c[c]:
                x.wait_recv()

            @pl.when(inner_high)
            def _():
                acc[w, :face] += nn(beside(d_r, w), opd[:, :face])
                send_down(c)

            @pl.when(last_slab)
            def _():
                acc[w, face:] += nn(beside(d_r, w), opd[:, face:])
                send_up(c)

        @pl.when(inner_high)
        def _():
            every = pl.ds(0, cols)
            acc[:, face:] += nn(beside(d_r, every), opd[:, face:])

        adj[:, :face] = adj[:, :face] - d_r[0].astype(F32)
        adj[:, :KMAX] = adj[:, :KMAX] + 0.5 * nn(d_r[1], zt_r[low_rows])
        adj[:, m - KMAX :] = adj[:, m - KMAX :] + 0.5 * nn(d_r[2], zr[low_rows])

    @pl.when(inner_high)
    def _():
        make_up()
        for c, w in enumerate(rows):
            for x in up_c[c]:
                x.wait_recv()

            @pl.when(inner_low)
            def _():
                acc[w, face:] += nn(beside(u_r, w), opu[...])
                send_up(c)

            adj[w, m - face :] = adj[w, m - face :] - u_r[0, w].astype(F32)
            adj[w, :KMAX] = adj[w, :KMAX] + 0.5 * nn(u_r[1, w], zt_r[high_rows])
            adj[w, m - KMAX :] = adj[w, m - KMAX :] + 0.5 * nn(u_r[2, w], zr[high_rows])

    out_ref[...] = halfway(adj[...].astype(BF), fac, m)

    for c in tail_c + head_c:
        c.wait_send()

    @pl.when(inner_low)
    def _():
        for c in zd_c:
            c.wait_send()
        for group in up_c:
            for x in group:
                x.wait_send()

    @pl.when(inner_high)
    def _():
        for c in zu_c:
            c.wait_send()
        for group in down_c:
            for x in group:
                x.wait_send()


def on_device(slabs, patches, right_side, inverse_factor, forward_trace, backward_trace, margin):
    cols, m = right_side.shape[2:]
    face = forward_trace.shape[2]
    parts = 4
    copies = 2 * parts + 4 + 6 * parts
    wide = pltpu.VMEM((cols, KMAX), BF)
    square = pltpu.VMEM((2 * face, KMAX), BF)
    thin = pltpu.VMEM((cols, face), BF)
    three = pltpu.VMEM((3, cols, face), BF)
    hbm = pl.BlockSpec(memory_space=pltpu.HBM)
    half = pl.pallas_call(
        functools.partial(kernel, slabs, patches, parts),
        out_shape=pltpu.VMEM((cols, m), BF),
        in_specs=[hbm, hbm, hbm, hbm, pl.BlockSpec(memory_space=pltpu.SMEM)],
        out_specs=pl.BlockSpec(memory_space=pltpu.VMEM),
        scratch_shapes=[
            pltpu.VMEM((cols, m), F32),
            pltpu.VMEM((m, m), BF),
            pltpu.VMEM((2 * face, m), BF),
            wide, wide, square, square, thin, thin,
            wide, wide, square, square, three, three,
            pltpu.VMEM((cols, m), F32),
            pltpu.VMEM((cols, 2 * face), F32),
            pltpu.VMEM((2 * face, m), BF),
            pltpu.VMEM((3 * face, 2 * face), BF),
            pltpu.VMEM((3 * face, face), BF),
            pltpu.VMEM((KMAX, KMAX), BF),
            square,
            pltpu.SemaphoreType.DMA((4,)),
            pltpu.SemaphoreType.DMA((copies,)),
            pltpu.SemaphoreType.DMA((copies,)),
        ],
        compiler_params=pltpu.CompilerParams(collective_id=0, has_side_effects=True),
        name="sweeps",
    )(right_side, inverse_factor, forward_trace, backward_trace, margin)
    return pl.pallas_call(
        finish,
        out_shape=jax.ShapeDtypeStruct(right_side.shape, F32),
        in_specs=[pl.BlockSpec(memory_space=pltpu.VMEM)] * 2,
        out_specs=hbm,
        scratch_shapes=[pltpu.VMEM((m // KMAX, cols, KMAX), F32), pltpu.SemaphoreType.DMA((m // KMAX,))],
        compiler_params=pltpu.CompilerParams(vmem_limit_bytes=16 << 20),
        name="finish",
    )(half, inverse_factor)


def solution(mesh):
    four = P("slab", "patch", None, None)
    return jax.shard_map(
        functools.partial(on_device, mesh.shape["slab"], mesh.shape["patch"]),
        mesh=mesh,
        in_specs=(four, four, four, four, P("slab", "patch")),
        out_specs=four,
        check_vma=False,
    )
```

```python
import functools

import jax
import jax.numpy as jnp
from jax import lax
from jax.experimental import pallas as pl
from jax.experimental.pallas import tpu as pltpu
from jax.sharding import PartitionSpec as P

KMAX = 256
BF = jnp.bfloat16
F32 = jnp.float32
MESH = pl.DeviceIdType.MESH


def nt(a, b):
    return lax.dot_general(a, b, (((1,), (1,)), ((), ())), preferred_element_type=F32)


def nn(a, b):
    return lax.dot_general(a, b, (((1,), (0,)), ((), ())), preferred_element_type=F32)


def tn(a, b):
    return lax.dot_general(a, b, (((0,), (0,)), ((), ())), preferred_element_type=F32)


def halfway(x, fac, m):
    return jnp.concatenate(
        [nt(x[:, : i + KMAX], fac[i : i + KMAX, : i + KMAX]).astype(BF) for i in range(0, m, KMAX)],
        axis=1,
    )


def solve(x, fac, m):
    half = halfway(x, fac, m)
    return [nn(half[:, k:], fac[k:, k : k + KMAX]) for k in range(0, m, KMAX)]


def finish(half_ref, l_ref, out_ref, held, sem):
    m = half_ref.shape[1]
    copies = []
    for n, k in enumerate(range(0, m, KMAX)):
        held[n] = nn(half_ref[:, k:], l_ref[0, 0, k:, k : k + KMAX])
        copies.append(pltpu.make_async_copy(held.at[n], out_ref.at[0, 0, :, k : k + KMAX], sem.at[n]))
        copies[-1].start()
    for c in copies:
        c.wait()


FAR_LEFT, FAR_RIGHT, LEFT, RIGHT, OWN = range(5)


class Names:
    def __init__(self):
        self.count = 0

    def take(self):
        self.count += 1
        return self.count - 1


def kernel(
    slabs, patches,
    r_hbm, l_hbm, f_hbm, b_hbm, margin_ref, out_ref,
    r_v, fac, maps,
    tail_s, head_s, zt_s, zh_s, d_s, a_s, b_s, t_s, v_s, w_s,
    tail_r, head_r, zt_r, zh_r, d_home, u_home,
    a_h, b_h, t_h, w_h, d_h, u_h, u0_s,
    adj, gt, place, zr,
    load_sem, send_sem, near_sem, home_sem, fed_sem, ring_sem, turn_sem,
):
    s = lax.axis_index("slab")
    q = lax.axis_index("patch")
    left = lax.rem(q + patches - 1, patches)
    right = lax.rem(q + 1, patches)
    m = fac.shape[-1]
    face = f_hbm.shape[-2]
    cols = r_v.shape[0]
    hosts = range(1, slabs, 2)
    wide = cols // len(hosts)
    inner_low, inner_high = s > 0, s < slabs - 1
    first_slab = s == 0
    pair = s + 1 - 2 * lax.rem(s, 2)
    host = lax.rem(s, 2) == 1
    next_left = lax.rem(q + patches - 2, patches)
    next_right = lax.rem(q + 2, patches)

    loads = [
        pltpu.make_async_copy(l_hbm.at[0, 0], fac, load_sem.at[1]),
        pltpu.make_async_copy(r_hbm.at[0, 0], r_v, load_sem.at[0]),
        pltpu.make_async_copy(f_hbm.at[0, 0], maps.at[:face], load_sem.at[2]),
        pltpu.make_async_copy(b_hbm.at[0, 0], maps.at[face:], load_sem.at[3]),
    ]
    for c in loads:
        c.start()

    barrier = pltpu.get_barrier_semaphore()

    def greet(slab, patch):
        pl.semaphore_signal(barrier, inc=1, device_id=(slab, patch), device_id_type=MESH)

    greet(s, left)
    greet(s, right)
    greet(pair, q)

    @pl.when(first_slab)
    def _():
        for h in hosts:
            for p in (left, q, right):
                greet(h, p)

    @pl.when(inner_low)
    def _():
        for h in hosts:
            @pl.when(s != h)
            def _():
                greet(h, q)

                @pl.when(host)
                def _():
                    greet(h, left)
                    greet(h, right)

    @pl.when(host)
    def _():
        greet(s, next_left)
        greet(s, next_right)
        for p in (left, q, right):
            greet(0, p)
        for t in range(1, slabs):
            @pl.when(s != t)
            def _():
                greet(t, q)

    here = host.astype(jnp.int32)
    greeted = (
        3
        + first_slab.astype(jnp.int32) * (3 * len(hosts))
        + inner_low.astype(jnp.int32) * len(hosts)
        + here * (2 * (len(hosts) - 1) + slabs + 2)
    )

    names = Names()

    def send(src, dst, recv, slab, patch):
        return pltpu.make_async_remote_copy(
            src_ref=src, dst_ref=dst, send_sem=send_sem.at[names.take()], recv_sem=recv,
            device_id=(slab, patch), device_id_type=MESH,
        )

    class Post:
        def __init__(self, here, src, dst, recv, slab, patch):
            self.here = here
            self.local = pltpu.make_async_copy(src, dst, recv)
            self.remote = send(src, dst, recv, slab, patch)

        def start(self):
            @pl.when(self.here)
            def _():
                self.local.start()

            @pl.when(~self.here)
            def _():
                self.remote.start()

        def wait_send(self):
            @pl.when(~self.here)
            def _():
                self.remote.wait_send()

    def arrived(dst, recv):
        pltpu.make_async_copy(dst, dst, recv).wait()

    part = [pl.ds(g * wide, wide) for g in range(len(hosts))]
    low_rows, high_rows = pl.ds(0, face), pl.ds(face, face)
    n_near = iter(range(64))
    tail_c = [send(tail_s.at[w], tail_r.at[w], near_sem.at[next(n_near)], s, right) for w in part]
    head_c = [send(head_s.at[w], head_r.at[w], near_sem.at[next(n_near)], s, left) for w in part]
    zd_c = [
        send(zt_s.at[low_rows], zt_r.at[low_rows], near_sem.at[next(n_near)], s, right),
        send(zh_s.at[low_rows], zh_r.at[low_rows], near_sem.at[next(n_near)], s, left),
    ]
    zu_c = [
        send(zt_s.at[high_rows], zt_r.at[high_rows], near_sem.at[next(n_near)], s, right),
        send(zh_s.at[high_rows], zh_r.at[high_rows], near_sem.at[next(n_near)], s, left),
    ]
    below = jnp.maximum(s - 1, 0)
    seed_c = [
        [send(d_s.at[w], d_h.at[0, j], ring_sem.at[0, 0], h, p) for j, p in ((LEFT, right), (RIGHT, left), (OWN, q))]
        for h, w in zip(hosts, part)
    ]
    t_c = [Post(s == h, t_s, t_h.at[below], fed_sem.at[0, below], h, q) for h in hosts]
    a_c = [Post(s == h, a_s.at[w], a_h.at[below], fed_sem.at[1, below], h, q) for h, w in zip(hosts, part)]

    def feed_up(src, dst, kind):
        own = [Post(s == h, x, dst.at[below, 2], fed_sem.at[kind, below], h, q) for h, x in zip(hosts, src)]
        near = [
            [send(x, dst.at[below, j], fed_sem.at[kind, below], h, p) for j, p in ((0, right), (1, left))]
            for h, x in zip(hosts, src)
        ]
        return own, near

    w_own, w_near = feed_up([w_s] * len(hosts), w_h, 2)
    b_own, b_near = feed_up([b_s.at[w] for w in part], b_h, 3)

    def start_up(own, near):
        own.start()

        @pl.when(host)
        def _():
            for c in near:
                c.start()

    group = s // 2
    back_d = [Post(s == t, d_h.at[t - 1, pl.ds(2, 3)], d_home.at[group], home_sem.at[0, group], t, q) for t in range(1, slabs)]
    back_u = [Post(s == t, u_h.at[t - 1, pl.ds(2, 3)], u_home.at[group], home_sem.at[1, group], t, q) for t in range(1, slabs - 1)]
    last_u = send(u0_s, u_home.at[group], home_sem.at[1, group], 0, q)

    def around(buf, n, kind, far):
        near = ((FAR_LEFT, next_right), (FAR_RIGHT, next_left)) if far else ()
        return [
            send(buf.at[n, OWN], buf.at[n, j], ring_sem.at[kind, n], s, p)
            for j, p in ((LEFT, right), (RIGHT, left)) + near
        ]

    round_d = {t: around(d_h, t - 1, 0, t == slabs - 1) for t in range(2, slabs)}
    round_u = {t: around(u_h, t - 1, 1, True) for t in range(1, slabs - 2, 2)}

    count = margin_ref[0, 0]
    row = lax.broadcasted_iota(jnp.int32, (KMAX, KMAX), 0)
    col = lax.broadcasted_iota(jnp.int32, (KMAX, KMAX), 1)
    hit = (row == KMAX - count + col) & (col < count)
    place[...] = jnp.where(hit, 1.0, 0.0).astype(BF)

    loads[0].wait()
    loads[1].wait()
    first = solve(r_v[...].astype(BF), fac, m)
    tail_s[...] = nn(first[-1].astype(BF), place[...]).astype(BF)
    head_s[...] = first[0].astype(BF)

    pl.semaphore_wait(barrier, greeted)

    def send_tails():
        for a, b in zip(tail_c, head_c):
            a.start()
            b.start()

    pl.when(first_slab)(send_tails)

    low = fac[:, :face]
    high = fac[m - face :, m - face :]
    k_tail = jnp.concatenate(
        [tn(low[m - KMAX :], fac[m - KMAX :, m - KMAX :]), tn(high, fac[m - face :, m - KMAX :])], axis=0
    )
    k_head = jnp.concatenate([tn(low, fac[:, :KMAX]), tn(high, fac[m - face :, :KMAX])], axis=0)
    zt_s[...] = nn(k_tail.astype(BF), place[...]).astype(BF)
    zh_s[...] = k_head.astype(BF)

    @pl.when(inner_low)
    def _():
        for c in zd_c:
            c.start()

        pl.when(~host)(send_tails)

    loads[2].wait()
    loads[3].wait()
    for k, piece in enumerate(solve(maps[...], fac, m)):
        gt[:, k * KMAX : (k + 1) * KMAX] = piece.astype(BF)

    @pl.when(~host)
    def _():
        for c in tail_c + head_c:
            c.wait_send()
        pl.semaphore_signal(turn_sem, inc=1, device_id=(pair, q), device_id_type=MESH)

    @pl.when(host)
    def _():
        pl.semaphore_wait(turn_sem, 1)
        send_tails()

    @pl.when(inner_low)
    def _():
        for c in zd_c:
            c.wait_recv()
        zr[low_rows] = nt(zh_r[low_rows], place[...]).astype(BF)
        own = (-gt[:, :face].astype(F32)).T.astype(BF)
        from_left = (0.5 * nt(zt_r[low_rows], gt[:, :KMAX])).astype(BF)
        from_right = (0.5 * nt(zr[low_rows], gt[:, m - KMAX :])).astype(BF)
        for n, block in enumerate((own, from_left, from_right)):
            t_s[n * face : (n + 1) * face, :] = block[:, :face]
            v_s[n * face : (n + 1) * face, :] = block[:, face:]

            @pl.when(~inner_high)
            def _():
                w_s[n * face : (n + 1) * face, :] = block[:, face:]

        @pl.when(inner_high)
        def _():
            for c in t_c:
                c.start()


    def pass_turn():
        pl.semaphore_signal(turn_sem, inc=1, device_id=(pair, q), device_id_type=MESH)

    def tails():
        for g, w in enumerate(part):
            tail_c[g].wait_recv()
            head_c[g].wait_recv()
            adj[w, :] = r_v[w, :]
            adj[w, :KMAX] = adj[w, :KMAX] - 0.5 * tail_r[w].astype(F32)
            adj[w, m - KMAX :] = adj[w, m - KMAX :] - 0.5 * nt(head_r[w], place[...])

            @pl.when(first_slab)
            def _():
                d_s[w] = nt(adj[w, :].astype(BF), gt[:face]).astype(BF)
                for c in seed_c[g]:
                    c.start()

            @pl.when(inner_low)
            def _():
                both = nt(adj[w, :].astype(BF), gt[...]).astype(BF)
                a_s[w] = both[:, :face]
                b_s[w] = both[:, face:]

                @pl.when(inner_high)
                def _():
                    a_c[g].start()

                @pl.when(~inner_high)
                def _():
                    start_up(b_own[g], b_near[g])

    @pl.when(host)
    def _():
        for c in tail_c + head_c:
            c.wait_send()

        @pl.when(inner_high)
        def _():
            for c in zu_c:
                c.start()

        pass_turn()

        @pl.when(~inner_high)
        def _():
            for own_c, near_c in zip(w_own, w_near):
                start_up(own_c, near_c)

    pl.when(s < 3)(tails)

    @pl.when(~host)
    def _():
        pl.when(s > 2)(tails)
        pl.semaphore_wait(turn_sem, 1)
        for c in zu_c:
            c.start()

    def make_up():
        for c in zu_c:
            c.wait_recv()
        zr[high_rows] = nt(zh_r[high_rows], place[...]).astype(BF)

        @pl.when(inner_low)
        def _():
            w_s[:face, :] = (-gt[face:, m - face :].astype(F32)).T.astype(BF)
            w_s[face : 2 * face, :] = (0.5 * nt(zt_r[high_rows], gt[face:, :KMAX])).astype(BF)
            w_s[2 * face :, :] = (0.5 * nt(zr[high_rows], gt[face:, m - KMAX :])).astype(BF)
            for own_c, near_c in zip(w_own, w_near):
                start_up(own_c, near_c)

    def beside(ref, n, slots):
        return jnp.concatenate([ref[n, j] for j in slots], axis=1)

    def take_down(g, w):
        arrived(d_home.at[g], home_sem.at[0, g])

        @pl.when(inner_high)
        def _():
            b_s[w] = (b_s[w].astype(F32) + nn(beside(d_home, g, (2, 0, 1)), v_s[...])).astype(BF)
            start_up(b_own[g], b_near[g])

    def drop_down():
        for g, w in enumerate(part):
            adj[w, :face] = adj[w, :face] - d_home[g, 2].astype(F32)
            adj[w, :KMAX] = adj[w, :KMAX] + 0.5 * nn(d_home[g, 0], zt_r[low_rows])
            adj[w, m - KMAX :] = adj[w, m - KMAX :] + 0.5 * nn(d_home[g, 1], zr[low_rows])

    @pl.when(inner_low & inner_high & ~host)
    def _():
        make_up()
        for g, w in enumerate(part):
            take_down(g, w)

    middle = (OWN, LEFT, RIGHT)

    @pl.when(host)
    def _():
        for t in range(1, slabs - 1):
            n = t - 1
            arrived(t_h.at[n], fed_sem.at[0, n])
            arrived(a_h.at[n], fed_sem.at[1, n])
            slots = d_h.at[n, pl.ds(2, 3 if t == 1 else 2)]
            arrived(slots, ring_sem.at[0, n])
            d_h[n + 1, OWN] = (a_h[n].astype(F32) + nn(beside(d_h, n, middle), t_h[n])).astype(BF)
            for c in round_d[t + 1]:
                c.start()
            back_d[n].start()
            if t == 1:
                pl.when(s > 1)(tails)

            @pl.when(s == t - 1)
            def _():
                make_up()
                for g, w in enumerate(part):
                    take_down(g, w)

        for t in range(slabs - 1, 0, -1):
            n = t - 1
            wide_step = t % 2 == 1
            top = t == slabs - 1
            state = d_h if top else u_h
            arrived(w_h.at[n] if wide_step else w_h.at[n, 2], fed_sem.at[2, n])
            arrived(b_h.at[n] if wide_step else b_h.at[n, 2], fed_sem.at[3, n])
            if wide_step:
                arrived(state.at[n, pl.ds(0, 4)], ring_sem.at[0 if top else 1, n])
            if wide_step:
                around_left, around_right = (LEFT, FAR_LEFT, OWN), (RIGHT, OWN, FAR_RIGHT)
                for j, slots in enumerate((around_left, around_right, middle)):
                    u = (b_h[n, j].astype(F32) + nn(beside(state, n, slots), w_h[n, j])).astype(BF)
                    if t > 1:
                        u_h[n - 1, 2 + j] = u
                    else:
                        u0_s[j] = u
                if t == 1:
                    last_u.start()
            else:
                u_h[n - 1, OWN] = (b_h[n, 2].astype(F32) + nn(beside(state, n, middle), w_h[n, 2])).astype(BF)
                for c in round_u[t - 1]:
                    c.start()
            if top:
                back_d[n].start()
            elif wide_step:
                back_u[n].start()
                back_u[n + 1].start()

    @pl.when(inner_low)
    def _():
        @pl.when(~inner_high)
        def _():
            for g, w in enumerate(part):
                take_down(g, w)

        drop_down()

    @pl.when(first_slab)
    def _():
        make_up()

    @pl.when(inner_high)
    def _():
        for g in range(len(hosts)):
            arrived(u_home.at[g], home_sem.at[1, g])
        for g, w in enumerate(part):
            adj[w, m - face :] = adj[w, m - face :] - u_home[g, 2].astype(F32)
            adj[w, :KMAX] = adj[w, :KMAX] + 0.5 * nn(u_home[g, 0], zt_r[high_rows])
            adj[w, m - KMAX :] = adj[w, m - KMAX :] + 0.5 * nn(u_home[g, 1], zr[high_rows])

    out_ref[...] = halfway(adj[...].astype(BF), fac, m)

    @pl.when(first_slab)
    def _():
        for group_c in seed_c:
            for c in group_c:
                c.wait_send()

    @pl.when(inner_low)
    def _():
        for c in zd_c + b_own + w_own:
            c.wait_send()

    @pl.when(inner_high)
    def _():
        for c in zu_c:
            c.wait_send()

    @pl.when(inner_low & inner_high)
    def _():
        for c in t_c + a_c:
            c.wait_send()

    @pl.when(host)
    def _():
        for c in back_d + back_u + [last_u]:
            c.wait_send()
        for near_c in w_near + b_near + list(round_d.values()) + list(round_u.values()):
            for c in near_c:
                c.wait_send()
    assert names.count <= send_sem.shape[0], names.count


def on_device(slabs, patches, right_side, inverse_factor, forward_trace, backward_trace, margin):
    cols, m = right_side.shape[2:]
    face = forward_trace.shape[2]
    groups = slabs // 2
    rows = cols // groups
    wide = pltpu.VMEM((cols, KMAX), BF)
    square = pltpu.VMEM((2 * face, KMAX), BF)
    thin = pltpu.VMEM((cols, face), BF)
    op = pltpu.VMEM((3 * face, face), BF)
    hbm = pl.BlockSpec(memory_space=pltpu.HBM)
    home = pltpu.VMEM((groups, 3, rows, face), BF)
    fed = pltpu.VMEM((slabs - 1, rows, face), BF)
    fed_up = pltpu.VMEM((slabs - 1, 3, rows, face), BF)
    ops = pltpu.VMEM((slabs - 1, 3 * face, face), BF)
    ops_up = pltpu.VMEM((slabs - 1, 3, 3 * face, face), BF)
    ring = pltpu.VMEM((slabs - 1, 5, rows, face), BF)
    sends = 13 * groups + 6 * slabs - 4
    half = pl.pallas_call(
        functools.partial(kernel, slabs, patches),
        out_shape=pltpu.VMEM((cols, m), BF),
        in_specs=[hbm, hbm, hbm, hbm, pl.BlockSpec(memory_space=pltpu.SMEM)],
        out_specs=pl.BlockSpec(memory_space=pltpu.VMEM),
        scratch_shapes=[
            pltpu.VMEM((cols, m), F32),
            pltpu.VMEM((m, m), BF),
            pltpu.VMEM((2 * face, m), BF),
            wide, wide, square, square, thin, thin, thin, op, op, op,
            wide, wide, square, square, home, home,
            fed, fed_up, ops, ops_up, ring, ring, pltpu.VMEM((3, rows, face), BF),
            pltpu.VMEM((cols, m), F32),
            pltpu.VMEM((2 * face, m), BF),
            pltpu.VMEM((KMAX, KMAX), BF),
            square,
            pltpu.SemaphoreType.DMA((4,)),
            pltpu.SemaphoreType.DMA((sends,)),
            pltpu.SemaphoreType.DMA((2 * groups + 4,)),
            pltpu.SemaphoreType.DMA((2, groups)),
            pltpu.SemaphoreType.DMA((4, slabs - 1)),
            pltpu.SemaphoreType.DMA((2, slabs - 1)),
            pltpu.SemaphoreType.REGULAR,
        ],
        compiler_params=pltpu.CompilerParams(collective_id=0, has_side_effects=True),
        name="sweeps",
    )(right_side, inverse_factor, forward_trace, backward_trace, margin)
    return pl.pallas_call(
        finish,
        out_shape=jax.ShapeDtypeStruct(right_side.shape, F32),
        in_specs=[pl.BlockSpec(memory_space=pltpu.VMEM)] * 2,
        out_specs=hbm,
        scratch_shapes=[pltpu.VMEM((m // KMAX, cols, KMAX), F32), pltpu.SemaphoreType.DMA((m // KMAX,))],
        compiler_params=pltpu.CompilerParams(vmem_limit_bytes=16 << 20),
        name="finish",
    )(half, inverse_factor)


def solution(mesh):
    four = P("slab", "patch", None, None)
    return jax.shard_map(
        functools.partial(on_device, mesh.shape["slab"], mesh.shape["patch"]),
        mesh=mesh,
        in_specs=(four, four, four, four, P("slab", "patch")),
        out_specs=four,
        check_vma=False,
    )
```

```python
import functools

import jax
import jax.numpy as jnp
from jax import lax
from jax.experimental import pallas as pl
from jax.experimental.pallas import tpu as pltpu
from jax.sharding import PartitionSpec as P

KMAX = 256
BF = jnp.bfloat16
F32 = jnp.float32
MESH = pl.DeviceIdType.MESH


def nt(a, b):
    return lax.dot_general(a, b, (((1,), (1,)), ((), ())), preferred_element_type=F32)


def nn(a, b):
    return lax.dot_general(a, b, (((1,), (0,)), ((), ())), preferred_element_type=F32)


def tn(a, b):
    return lax.dot_general(a, b, (((0,), (0,)), ((), ())), preferred_element_type=F32)


def halfway(x, fac, m):
    return jnp.concatenate(
        [nt(x[:, : i + KMAX], fac[i : i + KMAX, : i + KMAX]).astype(BF) for i in range(0, m, KMAX)],
        axis=1,
    )


def solve(x, fac, m):
    half = halfway(x, fac, m)
    return [nn(half[:, k:], fac[k:, k : k + KMAX]) for k in range(0, m, KMAX)]


def finish(half_ref, l_ref, out_ref, held, sem):
    m = half_ref.shape[1]
    copies = []
    for n, k in enumerate(range(0, m, KMAX)):
        held[n] = nn(half_ref[:, k:], l_ref[0, 0, k:, k : k + KMAX])
        copies.append(pltpu.make_async_copy(held.at[n], out_ref.at[0, 0, :, k : k + KMAX], sem.at[n]))
        copies[-1].start()
    for c in copies:
        c.wait()


FAR_LEFT, FAR_RIGHT, LEFT, RIGHT, OWN = range(5)
HOST, AIDE = 1, 2


class Names:
    def __init__(self):
        self.count = 0

    def take(self):
        self.count += 1
        return self.count - 1


def kernel(
    slabs, patches, halves,
    r_hbm, l_hbm, f_hbm, b_hbm, margin_ref, out_ref,
    r_v, fac, maps,
    tail_s, head_s, zt_s, zh_s, d_s,
    side_r, z_r, d_home, u_home,
    a_h, b_h, t_h, v_h, w_h, d_h, u_h, u0_s,
    adj, gt, place, zr, lent,
    load_sem, send_sem, near_sem, home_sem, op_sem, term_sem, ring_sem, aide_sem, turn_sem,
):
    s = lax.axis_index("slab")
    q = lax.axis_index("patch")
    left = lax.rem(q + patches - 1, patches)
    right = lax.rem(q + 1, patches)
    next_left = lax.rem(q + patches - 2, patches)
    next_right = lax.rem(q + 2, patches)
    pair = s + 1 - 2 * lax.rem(s, 2)
    odd = lax.rem(s, 2) == 1
    m = fac.shape[-1]
    face = f_hbm.shape[-2]
    cols = r_v.shape[0]
    top = slabs - 1
    wide = cols // halves
    inner_low, inner_high = s > 0, s < top
    first_slab = s == 0
    host, guest, last = s == HOST, s > HOST, s == top
    odd_guest = guest & odd
    aide = s == AIDE

    loads = [
        pltpu.make_async_copy(l_hbm.at[0, 0], fac, load_sem.at[1]),
        pltpu.make_async_copy(r_hbm.at[0, 0], r_v, load_sem.at[0]),
        pltpu.make_async_copy(f_hbm.at[0, 0], maps.at[:face], load_sem.at[2]),
        pltpu.make_async_copy(b_hbm.at[0, 0], maps.at[face:], load_sem.at[3]),
    ]
    for c in loads:
        c.start()

    barrier = pltpu.get_barrier_semaphore()

    def greet(slab, patch):
        pl.semaphore_signal(barrier, inc=1, device_id=(slab, patch), device_id_type=MESH)

    greet(s, left)
    greet(s, right)
    greet(pair, q)

    @pl.when(first_slab)
    def _():
        greet(HOST, left)
        greet(HOST, right)
        greet(AIDE, q)

    @pl.when(aide)
    def _():
        greet(0, q)

    @pl.when(guest)
    def _():
        greet(HOST, q)

    @pl.when(odd_guest)
    def _():
        greet(HOST, left)
        greet(HOST, right)

    @pl.when(host)
    def _():
        greet(s, next_left)
        greet(s, next_right)
        greet(0, left)
        greet(0, right)
        for t in range(HOST + 1, slabs):
            greet(t, q)
        for t in range(HOST + 2, slabs, 2):
            greet(t, left)
            greet(t, right)

    greeted = (
        3
        + first_slab.astype(jnp.int32) * 3
        + aide.astype(jnp.int32)
        + guest.astype(jnp.int32)
        + odd_guest.astype(jnp.int32) * 2
        + host.astype(jnp.int32) * (4 + slabs - 2 + 2 * len(range(HOST + 2, slabs, 2)))
    )

    names = Names()

    class Group:
        def __init__(self, whole, copies):
            self.whole, self.sem = whole, send_sem.at[names.take()]
            self.copies = [
                pltpu.make_async_remote_copy(
                    src_ref=src, dst_ref=dst, send_sem=self.sem, recv_sem=recv, device_id=place, device_id_type=MESH
                )
                for src, dst, recv, place in copies
            ]

        def start(self, first=0, end=None):
            for c in self.copies[first:end]:
                c.start()

        def sent(self):
            arrived(self.whole, self.sem)

    def arrived(ref, sem):
        pltpu.make_async_copy(ref, ref, sem).wait()

    def start(*groups):
        for c in groups:
            c.start()

    def sent(*groups):
        for c in groups:
            c.sent()

    part = [pl.ds(g * wide, wide) for g in range(halves)]
    both = range(halves)
    low_rows, high_rows = pl.ds(0, face), pl.ds(face, face)
    two, four, middle = pl.ds(0, 2), pl.ds(0, 4), pl.ds(2, 3)

    tail_c = [
        Group(
            tail_s,
            [
                (tail_s.at[w], side_r.at[0, w], near_sem.at[g], (s, right)),
                (head_s.at[w], side_r.at[1, w], near_sem.at[g], (s, left)),
            ],
        )
        for g, w in enumerate(part)
    ]

    def z_rows(rows, n):
        return Group(
            zt_s,
            [
                (zt_s.at[rows], z_r.at[0, rows], near_sem.at[halves + n], (s, right)),
                (zh_s.at[rows], z_r.at[1, rows], near_sem.at[halves + n], (s, left)),
            ],
        )

    zd_c, zu_c = z_rows(low_rows, 0), z_rows(high_rows, 1)
    shared = names.count

    seed_c = Group(
        d_h.at[0, :, middle],
        [
            (d_s.at[w], d_h.at[0, g, j], ring_sem.at[g], (HOST, p))
            for g, w in enumerate(part)
            for j, p in ((LEFT, right), (RIGHT, left), (OWN, q))
        ],
    )
    lent_c = Group(
        zt_s,
        [
            (zt_s.at[high_rows], lent.at[0], aide_sem.at[0], (AIDE, q)),
            (zh_s.at[high_rows], lent.at[1], aide_sem.at[0], (AIDE, q)),
        ],
    )
    most = names.count

    names.count = shared
    below = jnp.maximum(s - 1, 0)
    inner = jnp.maximum(s - 2, 0)
    inners = slabs - 3
    sides = ((0, right), (1, left))
    t_sem, v_sem, w_sem = 0, inners, 2 * inners
    a_sem, b_sem, k_sem = 0, halves * inners, halves * inners + slabs - 2
    t_c = Group(t_h.at[below], [(t_h.at[below], t_h.at[below], op_sem.at[t_sem + inner], (HOST, q))])
    v_c = Group(v_h.at[below], [(v_h.at[below], v_h.at[below], op_sem.at[v_sem + inner], (HOST, q))])
    w_to = op_sem.at[w_sem + below]
    w_c = Group(w_h.at[below, 2], [(w_h.at[below, 2], w_h.at[below, 2], w_to, (HOST, q))])
    w_near = Group(w_h.at[below, two], [(w_h.at[below, 2], w_h.at[below, j], w_to, (HOST, p)) for j, p in sides])
    a_c = Group(
        a_h.at[below],
        [(a_h.at[below, g], a_h.at[below, g], term_sem.at[a_sem + halves * inner + g], (HOST, q)) for g in both],
    )
    b_to = term_sem.at[b_sem + inner]
    b_c = Group(b_h.at[below, :, 2], [(b_h.at[below, g, 2], b_h.at[below, g, 2], b_to, (HOST, q)) for g in both])
    b_swap = Group(
        b_h.at[below, :, two],
        [(b_h.at[below, g, 2], b_h.at[below, g, j], near_sem.at[halves + 2], (s, p)) for g in both for j, p in sides],
    )
    b_pass = Group(
        b_h.at[below, :, two],
        [(b_h.at[below, :, two], b_h.at[below, :, two], b_to, (HOST, q))],
    )
    lent_near = Group(
        lent.at[two],
        [
            (lent.at[0], lent.at[2], aide_sem.at[1], (AIDE, right)),
            (lent.at[1], lent.at[3], aide_sem.at[1], (AIDE, left)),
        ],
    )
    lent_back = Group(
        lent.at[two],
        [(lent.at[2 + n], z_r.at[n, high_rows], near_sem.at[halves + 1], (0, q)) for n in range(2)],
    )
    most = max(most, names.count)

    names.count = shared
    close = ((LEFT, right), (RIGHT, left))
    far = close + ((FAR_LEFT, next_right), (FAR_RIGHT, next_left))
    up_rings = range(1, top - 1, 2)

    def ring_of(kind, t):
        return halves * (t - 1) if kind == 0 else halves * (slabs - 1 + up_rings.index(t))

    def around(buf, t, kind, places):
        return Group(
            buf.at[t - 1, :, pl.ds(0, len(places))],
            [
                (buf.at[t - 1, g, OWN], buf.at[t - 1, g, j], ring_sem.at[ring_of(kind, t) + g], (s, p))
                for g in both
                for j, p in places
            ],
        )

    round_d = {t: around(d_h, t, 0, far if t == top else close) for t in range(2, slabs)}
    round_u = {t: around(u_h, t, 1, far) for t in up_rings}
    kept_c = {
        t: Group(
            b_h.at[t - 1, :, two],
            [
                (b_h.at[t - 1, g, 2], b_h.at[t - 1, g, j], term_sem.at[k_sem + t // 2], (s, p))
                for g in both
                for j, p in sides
            ],
        )
        for t in range(1, top, 2)
    }
    w_host = Group(w_h.at[0, two], [(w_h.at[0, 2], w_h.at[0, j], op_sem.at[w_sem], (s, p)) for j, p in sides])

    def back(src, dst, recv, t):
        return Group(src, [(src, dst, recv, (t, q))])

    back_d = {t: back(d_h.at[t - 1, :, middle], d_home, home_sem.at[0], t) for t in range(2, slabs)}
    back_u = {t: back(u_h.at[t - 1, :, middle], u_home, home_sem.at[1], t) for t in range(2, top)}
    last_u = Group(u0_s, [(u0_s.at[g], u_home.at[g], home_sem.at[1 + g], (0, q)) for g in both])
    most = max(most, names.count)
    assert most == send_sem.shape[0], most

    count = margin_ref[0, 0]
    row = lax.broadcasted_iota(jnp.int32, (KMAX, KMAX), 0)
    col = lax.broadcasted_iota(jnp.int32, (KMAX, KMAX), 1)
    hit = (row == KMAX - count + col) & (col < count)
    place[...] = jnp.where(hit, 1.0, 0.0).astype(BF)

    loads[0].wait()
    loads[1].wait()
    first = solve(r_v[...].astype(BF), fac, m)
    tail_s[...] = nn(first[-1].astype(BF), place[...]).astype(BF)
    head_s[...] = first[0].astype(BF)

    pl.semaphore_wait(barrier, greeted)

    def send_tails():
        start(*tail_c)

    pl.when(first_slab)(send_tails)

    low = fac[:, :face]
    high = fac[m - face :, m - face :]
    k_tail = jnp.concatenate(
        [tn(low[m - KMAX :], fac[m - KMAX :, m - KMAX :]), tn(high, fac[m - face :, m - KMAX :])], axis=0
    )
    k_head = jnp.concatenate([tn(low, fac[:, :KMAX]), tn(high, fac[m - face :, :KMAX])], axis=0)
    zt_s[...] = nn(k_tail.astype(BF), place[...]).astype(BF)
    zh_s[...] = k_head.astype(BF)

    @pl.when(inner_low)
    def _():
        start(zd_c)
        pl.when(guest)(send_tails)

    loads[2].wait()
    loads[3].wait()
    for k, piece in enumerate(solve(maps[...], fac, m)):
        gt[:, k * KMAX : (k + 1) * KMAX] = piece.astype(BF)

    @pl.when(first_slab)
    def _():
        tail_c[0].sent()
        pl.semaphore_signal(turn_sem, inc=1, device_id=(HOST, q), device_id_type=MESH)

    @pl.when(host)
    def _():
        pl.semaphore_wait(turn_sem, 1)
        send_tails()

    @pl.when(inner_low)
    def _():
        arrived(z_r.at[:, low_rows], near_sem.at[halves])
        zr[low_rows] = nt(z_r[1, low_rows], place[...]).astype(BF)
        own = (-gt[:, :face].astype(F32)).T.astype(BF)
        from_left = (0.5 * nt(z_r[0, low_rows], gt[:, :KMAX])).astype(BF)
        from_right = (0.5 * nt(zr[low_rows], gt[:, m - KMAX :])).astype(BF)
        for n, block in enumerate((own, from_left, from_right)):
            lines = pl.ds(n * face, face)
            t_h[below, lines] = block[:, :face]

            @pl.when(inner_high)
            def _():
                v_h[below, lines] = block[:, face:]

            @pl.when(~inner_high)
            def _():
                w_h[below, 2, lines] = block[:, face:]

        @pl.when(guest & inner_high)
        def _():
            start(t_c, v_c)

        @pl.when(last)
        def _():
            start(w_c)

    for g, w in enumerate(part):
        arrived(side_r.at[:, w], near_sem.at[g])
        adj[w, :] = r_v[w, :]
        adj[w, :KMAX] = adj[w, :KMAX] - 0.5 * side_r[0, w].astype(F32)
        adj[w, m - KMAX :] = adj[w, m - KMAX :] - 0.5 * nt(side_r[1, w], place[...])

        @pl.when(first_slab)
        def _():
            d_s[w] = nt(adj[w, :].astype(BF), gt[:face]).astype(BF)
            seed_c.start(3 * g, 3 * g + 3)

        @pl.when(inner_low)
        def _():
            terms = nt(adj[w, :].astype(BF), gt[...]).astype(BF)
            a_h[below, g] = terms[:, :face]
            b_h[below, g, 2] = terms[:, face:]

            @pl.when(guest & inner_high)
            def _():
                a_c.start(g, g + 1)

            @pl.when(guest)
            def _():
                b_c.start(g, g + 1)

            @pl.when(last)
            def _():
                b_swap.start(2 * g, 2 * g + 2)

    @pl.when(last)
    def _():
        start(w_near)
        arrived(b_h.at[below, :, two], near_sem.at[halves + 2])
        start(b_pass)

    @pl.when(first_slab)
    def _():
        start(lent_c)

    @pl.when(guest & inner_high)
    def _():
        start(zu_c)

    def make_up():
        arrived(z_r.at[:, high_rows], near_sem.at[halves + 1])
        zr[high_rows] = nt(z_r[1, high_rows], place[...]).astype(BF)

        @pl.when(inner_low)
        def _():
            w_h[below, 2, :face] = (-gt[face:, m - face :].astype(F32)).T.astype(BF)
            w_h[below, 2, face : 2 * face] = (0.5 * nt(z_r[0, high_rows], gt[face:, :KMAX])).astype(BF)
            w_h[below, 2, 2 * face :] = (0.5 * nt(zr[high_rows], gt[face:, m - KMAX :])).astype(BF)

    @pl.when(guest & inner_high)
    def _():
        make_up()
        start(w_c)

        @pl.when(odd)
        def _():
            start(w_near)

    @pl.when(aide)
    def _():
        arrived(lent.at[two], aide_sem.at[0])
        start(lent_near)
        arrived(lent.at[pl.ds(2, 2)], aide_sem.at[1])
        start(lent_back)

    def beside(ref, n, g, slots):
        return jnp.concatenate([ref[n, g, j] for j in slots], axis=1)

    centre = (OWN, LEFT, RIGHT)

    @pl.when(host)
    def _():
        for t in range(1, top):
            n = t - 1
            if t > HOST:
                arrived(t_h.at[n], op_sem.at[t_sem + n - 1])
            for g in both:
                if t > HOST:
                    arrived(a_h.at[n, g], term_sem.at[a_sem + halves * (n - 1) + g])
                arrived(d_h.at[n, g, pl.ds(2, 3 if t == 1 else 2)], ring_sem.at[ring_of(0, t) + g])
                d_h[n + 1, g, OWN] = (a_h[n, g].astype(F32) + nn(beside(d_h, n, g, centre), t_h[n])).astype(BF)
                per = len(far if t + 1 == top else close)
                round_d[t + 1].start(per * g, per * g + per)
            if t == 1:
                start(zu_c)
            if t > HOST:
                back_d[t].start()
                arrived(v_h.at[n], op_sem.at[v_sem + n - 1])
                arrived(b_h.at[n, :, 2], term_sem.at[b_sem + n - 1])
            for g in both:
                b_h[n, g, 2] = (b_h[n, g, 2].astype(F32) + nn(beside(d_h, n, g, centre), v_h[n])).astype(BF)
                if t % 2 == 1:
                    kept_c[t].start(2 * g, 2 * g + 2)
            if t == min(2, top - 1):
                make_up()
                start(w_host)

        arrived(w_h.at[top - 1], op_sem.at[w_sem + top - 1])
        for t in range(top, 0, -2):
            n = t - 1
            state = d_h if t == top else u_h
            if t < top:
                arrived(w_h.at[n, two] if t == HOST else w_h.at[n], op_sem.at[w_sem + n])
            if t > 1:
                arrived(w_h.at[n - 1, 2], op_sem.at[w_sem + n - 1])
            if t == top:
                arrived(b_h.at[n], term_sem.at[b_sem + n - 1])
            else:
                arrived(b_h.at[n, :, two], term_sem.at[k_sem + t // 2])
            for g in both:
                arrived(state.at[n, g, four], ring_sem.at[ring_of(0 if t == top else 1, t) + g])
                for j, slots in enumerate(((LEFT, FAR_LEFT, OWN), (RIGHT, OWN, FAR_RIGHT), centre)):
                    u = (b_h[n, g, j].astype(F32) + nn(beside(state, n, g, slots), w_h[n, j])).astype(BF)
                    if t > 1:
                        u_h[n - 1, g, 2 + j] = u
                    else:
                        u0_s[g, j] = u
                if t > 1:
                    u = b_h[n - 1, g, 2].astype(F32) + nn(beside(u_h, n - 1, g, centre), w_h[n - 1, 2])
                    u_h[n - 2, g, OWN] = u.astype(BF)
                    round_u[t - 2].start(4 * g, 4 * g + 4)
                else:
                    last_u.start(g, g + 1)
            if t == top:
                back_d[t].start()
            elif t > HOST:
                back_u[t].start()
            if t > 1:
                back_u[t - 1].start()

    def drop_low(get):
        for g, w in enumerate(part):
            adj[w, :face] = adj[w, :face] - get(g, 2).astype(F32)
            adj[w, :KMAX] = adj[w, :KMAX] + 0.5 * nn(get(g, 0), z_r[0, low_rows])
            adj[w, m - KMAX :] = adj[w, m - KMAX :] + 0.5 * nn(get(g, 1), zr[low_rows])

    def drop_high(g, get):
        w = part[g]
        adj[w, m - face :] = adj[w, m - face :] - get(g, 2).astype(F32)
        adj[w, :KMAX] = adj[w, :KMAX] + 0.5 * nn(get(g, 0), z_r[0, high_rows])
        adj[w, m - KMAX :] = adj[w, m - KMAX :] + 0.5 * nn(get(g, 1), zr[high_rows])

    @pl.when(host)
    def _():
        drop_low(lambda g, j: d_h[0, g, 2 + j])
        if HOST < top:
            for g in both:
                drop_high(g, lambda g, j: u_h[0, g, 2 + j])

    @pl.when(guest)
    def _():
        arrived(d_home, home_sem.at[0])
        drop_low(lambda g, j: d_home[g, j])

    @pl.when(guest & inner_high)
    def _():
        arrived(u_home, home_sem.at[1])
        for g in both:
            drop_high(g, lambda g, j: u_home[g, j])

    @pl.when(first_slab)
    def _():
        make_up()
        for g in both:
            arrived(u_home.at[g], home_sem.at[1 + g])
            drop_high(g, lambda g, j: u_home[g, j])

    out_ref[...] = halfway(adj[...].astype(BF), fac, m)

    @pl.when(first_slab)
    def _():
        sent(tail_c[1], lent_c, seed_c)

    @pl.when(inner_low)
    def _():
        sent(zd_c, *tail_c)

    @pl.when(inner_low & inner_high)
    def _():
        sent(zu_c)

    @pl.when(aide)
    def _():
        sent(lent_near, lent_back)

    @pl.when(guest)
    def _():
        sent(w_c, b_c)

    @pl.when(guest & inner_high)
    def _():
        sent(t_c, v_c, a_c)

    @pl.when(odd_guest)
    def _():
        sent(w_near)

    @pl.when(last)
    def _():
        sent(b_swap, b_pass)

    @pl.when(host)
    def _():
        sent(w_host, last_u)
        for kind in (round_d, round_u, kept_c, back_d, back_u):
            sent(*kind.values())


def on_device(slabs, patches, right_side, inverse_factor, forward_trace, backward_trace, margin):
    cols, m = right_side.shape[2:]
    face = forward_trace.shape[2]
    halves = 2
    rows = cols // halves
    links = slabs - 1
    wide = pltpu.VMEM((cols, KMAX), BF)
    square = pltpu.VMEM((2 * face, KMAX), BF)
    hbm = pl.BlockSpec(memory_space=pltpu.HBM)
    home = pltpu.VMEM((halves, 3, rows, face), BF)
    ops = pltpu.VMEM((links, 3 * face, face), BF)
    ring = pltpu.VMEM((links, halves, 5, rows, face), BF)
    sends = halves + 2 + max(10, 2 * (links - 1) + (links - 2) + 3 * (slabs // 2 - 1) - (slabs // 2 - 1) + 2)
    half = pl.pallas_call(
        functools.partial(kernel, slabs, patches, halves),
        out_shape=pltpu.VMEM((cols, m), BF),
        in_specs=[hbm, hbm, hbm, hbm, pl.BlockSpec(memory_space=pltpu.SMEM)],
        out_specs=pl.BlockSpec(memory_space=pltpu.VMEM),
        scratch_shapes=[
            pltpu.VMEM((cols, m), F32),
            pltpu.VMEM((m, m), BF),
            pltpu.VMEM((2 * face, m), BF),
            wide, wide, square, square, pltpu.VMEM((cols, face), BF),
            pltpu.VMEM((2, cols, KMAX), BF), pltpu.VMEM((2, 2 * face, KMAX), BF), home, home,
            pltpu.VMEM((links, halves, rows, face), BF),
            pltpu.VMEM((links, halves, 3, rows, face), BF),
            ops, ops, pltpu.VMEM((links, 3, 3 * face, face), BF),
            ring, ring, home,
            pltpu.VMEM((cols, m), F32),
            pltpu.VMEM((2 * face, m), BF),
            pltpu.VMEM((KMAX, KMAX), BF),
            square,
            pltpu.VMEM((4, face, KMAX), BF),
            pltpu.SemaphoreType.DMA((4,)),
            pltpu.SemaphoreType.DMA((sends,)),
            pltpu.SemaphoreType.DMA((halves + 3,)),
            pltpu.SemaphoreType.DMA((1 + halves,)),
            pltpu.SemaphoreType.DMA((2 * (links - 2) + links,)),
            pltpu.SemaphoreType.DMA((halves * (links - 2) + links - 1 + slabs // 2 - 1,)),
            pltpu.SemaphoreType.DMA((halves * (links + slabs // 2 - 1),)),
            pltpu.SemaphoreType.DMA((2,)),
            pltpu.SemaphoreType.REGULAR,
        ],
        compiler_params=pltpu.CompilerParams(collective_id=0, has_side_effects=True),
        name="sweeps",
    )(right_side, inverse_factor, forward_trace, backward_trace, margin)
    return pl.pallas_call(
        finish,
        out_shape=jax.ShapeDtypeStruct(right_side.shape, F32),
        in_specs=[pl.BlockSpec(memory_space=pltpu.VMEM)] * 2,
        out_specs=hbm,
        scratch_shapes=[pltpu.VMEM((m // KMAX, cols, KMAX), F32), pltpu.SemaphoreType.DMA((m // KMAX,))],
        compiler_params=pltpu.CompilerParams(vmem_limit_bytes=16 << 20),
        name="finish",
    )(half, inverse_factor)


def solution(mesh):
    four = P("slab", "patch", None, None)
    return jax.shard_map(
        functools.partial(on_device, mesh.shape["slab"], mesh.shape["patch"]),
        mesh=mesh,
        in_specs=(four, four, four, four, P("slab", "patch")),
        out_specs=four,
        check_vma=False,
    )
```

```python
import functools

import jax
import jax.numpy as jnp
from jax import lax
from jax.experimental import pallas as pl
from jax.experimental.pallas import tpu as pltpu
from jax.sharding import PartitionSpec as P

KMAX = 256
BF = jnp.bfloat16
F32 = jnp.float32
MESH = pl.DeviceIdType.MESH


def nt(a, b):
    return lax.dot_general(a, b, (((1,), (1,)), ((), ())), preferred_element_type=F32)


def nn(a, b):
    return lax.dot_general(a, b, (((1,), (0,)), ((), ())), preferred_element_type=F32)


def tn(a, b):
    return lax.dot_general(a, b, (((0,), (0,)), ((), ())), preferred_element_type=F32)


def halfway(x, fac, m):
    return jnp.concatenate(
        [nt(x[:, : i + KMAX], fac[i : i + KMAX, : i + KMAX]).astype(BF) for i in range(0, m, KMAX)],
        axis=1,
    )


def solve(x, fac, m):
    half = halfway(x, fac, m)
    return [nn(half[:, k:], fac[k:, k : k + KMAX]) for k in range(0, m, KMAX)]


def finish(half_ref, l_ref, out_ref, held, sem):
    m = half_ref.shape[1]
    copies = []
    for n, k in enumerate(range(0, m, KMAX)):
        held[n] = nn(half_ref[:, k:], l_ref[0, 0, k:, k : k + KMAX])
        copies.append(pltpu.make_async_copy(held.at[n], out_ref.at[0, 0, :, k : k + KMAX], sem.at[n]))
        copies[-1].start()
    for c in copies:
        c.wait()


FAR_LEFT, FAR_RIGHT, LEFT, RIGHT, OWN = range(5)
HOST, AIDE = 1, 2


class Names:
    def __init__(self):
        self.count = 0

    def take(self):
        self.count += 1
        return self.count - 1


def kernel(
    slabs, patches, halves,
    r_hbm, l_hbm, f_hbm, b_hbm, margin_ref, out_ref,
    r_v, fac, maps,
    tail_s, head_s, zt_s, zh_s, d_s,
    side_r, z_r, d_home, u_home,
    a_h, b_h, t_h, v_h, w_h, d_h, u_h, u0_s,
    adj, gt, place, zr, lent,
    load_sem, send_sem, near_sem, home_sem, op_sem, term_sem, ring_sem, aide_sem, turn_sem,
):
    s = lax.axis_index("slab")
    q = lax.axis_index("patch")
    left = lax.rem(q + patches - 1, patches)
    right = lax.rem(q + 1, patches)
    next_left = lax.rem(q + patches - 2, patches)
    next_right = lax.rem(q + 2, patches)
    pair = s + 1 - 2 * lax.rem(s, 2)
    odd = lax.rem(s, 2) == 1
    m = fac.shape[-1]
    face = f_hbm.shape[-2]
    cols = r_v.shape[0]
    top = slabs - 1
    wide = cols // halves
    inner_low, inner_high = s > 0, s < top
    first_slab = s == 0
    host, guest, last = s == HOST, s > HOST, s == top
    odd_guest = guest & odd
    aide = s == AIDE

    loads = [
        pltpu.make_async_copy(l_hbm.at[0, 0], fac, load_sem.at[1]),
        pltpu.make_async_copy(r_hbm.at[0, 0], r_v, load_sem.at[0]),
        pltpu.make_async_copy(f_hbm.at[0, 0], maps.at[:face], load_sem.at[2]),
        pltpu.make_async_copy(b_hbm.at[0, 0], maps.at[face:], load_sem.at[3]),
    ]
    for c in loads:
        c.start()

    barrier = pltpu.get_barrier_semaphore()

    def greet(slab, patch):
        pl.semaphore_signal(barrier, inc=1, device_id=(slab, patch), device_id_type=MESH)

    greet(s, left)
    greet(s, right)
    greet(pair, q)

    @pl.when(first_slab)
    def _():
        greet(HOST, left)
        greet(HOST, right)
        greet(AIDE, q)

    @pl.when(aide)
    def _():
        greet(0, q)

    @pl.when(guest)
    def _():
        greet(HOST, q)

    @pl.when(odd_guest)
    def _():
        greet(HOST, left)
        greet(HOST, right)

    @pl.when(host)
    def _():
        greet(s, next_left)
        greet(s, next_right)
        greet(0, left)
        greet(0, right)
        for t in range(HOST + 1, slabs):
            greet(t, q)
        for t in range(HOST + 2, slabs, 2):
            greet(t, left)
            greet(t, right)

    greeted = (
        3
        + first_slab.astype(jnp.int32) * 3
        + aide.astype(jnp.int32)
        + guest.astype(jnp.int32)
        + odd_guest.astype(jnp.int32) * 2
        + host.astype(jnp.int32) * (4 + slabs - 2 + 2 * len(range(HOST + 2, slabs, 2)))
    )

    names = Names()

    class Group:
        def __init__(self, whole, copies):
            self.whole, self.sem = whole, send_sem.at[names.take()]
            self.copies = [
                pltpu.make_async_remote_copy(
                    src_ref=src, dst_ref=dst, send_sem=self.sem, recv_sem=recv, device_id=place, device_id_type=MESH
                )
                for src, dst, recv, place in copies
            ]

        def start(self, first=0, end=None):
            for c in self.copies[first:end]:
                c.start()

        def sent(self):
            arrived(self.whole, self.sem)

    def arrived(ref, sem):
        pltpu.make_async_copy(ref, ref, sem).wait()

    def start(*groups):
        for c in groups:
            c.start()

    def sent(*groups):
        for c in groups:
            c.sent()

    part = [pl.ds(g * wide, wide) for g in range(halves)]
    both = range(halves)
    low_rows, high_rows = pl.ds(0, face), pl.ds(face, face)
    two, four, middle = pl.ds(0, 2), pl.ds(0, 4), pl.ds(2, 3)

    tail_c = [
        Group(
            tail_s,
            [
                (tail_s.at[w], side_r.at[0, w], near_sem.at[g], (s, right)),
                (head_s.at[w], side_r.at[1, w], near_sem.at[g], (s, left)),
            ],
        )
        for g, w in enumerate(part)
    ]

    def z_rows(rows, n):
        return Group(
            zt_s,
            [
                (zt_s.at[rows], z_r.at[0, rows], near_sem.at[halves + n], (s, right)),
                (zh_s.at[rows], z_r.at[1, rows], near_sem.at[halves + n], (s, left)),
            ],
        )

    zd_c, zu_c = z_rows(low_rows, 0), z_rows(high_rows, 1)
    shared = names.count

    seed_c = Group(
        d_h.at[0, :, middle],
        [
            (d_s.at[w], d_h.at[0, g, j], ring_sem.at[g], (HOST, p))
            for g, w in enumerate(part)
            for j, p in ((LEFT, right), (RIGHT, left), (OWN, q))
        ],
    )
    lent_c = Group(
        zt_s,
        [
            (zt_s.at[high_rows], lent.at[0], aide_sem.at[0], (AIDE, q)),
            (zh_s.at[high_rows], lent.at[1], aide_sem.at[0], (AIDE, q)),
        ],
    )
    most = names.count

    names.count = shared
    below = jnp.maximum(s - 1, 0)
    inner = jnp.maximum(s - 2, 0)
    inners = slabs - 3
    sides = ((0, right), (1, left))
    t_sem, v_sem, w_sem = 0, inners, 2 * inners
    a_sem, b_sem, k_sem = 0, halves * inners, halves * inners + slabs - 2
    t_c = Group(t_h.at[below], [(t_h.at[below], t_h.at[below], op_sem.at[t_sem + inner], (HOST, q))])
    v_c = Group(v_h.at[below], [(v_h.at[below], v_h.at[below], op_sem.at[v_sem + inner], (HOST, q))])
    w_to = op_sem.at[w_sem + below]
    w_c = Group(w_h.at[below, 2], [(w_h.at[below, 2], w_h.at[below, 2], w_to, (HOST, q))])
    w_near = Group(w_h.at[below, two], [(w_h.at[below, 2], w_h.at[below, j], w_to, (HOST, p)) for j, p in sides])
    a_c = Group(
        a_h.at[below],
        [(a_h.at[below, g], a_h.at[below, g], term_sem.at[a_sem + halves * inner + g], (HOST, q)) for g in both],
    )
    b_to = term_sem.at[b_sem + inner]
    b_c = Group(b_h.at[below, :, 2], [(b_h.at[below, g, 2], b_h.at[below, g, 2], b_to, (HOST, q)) for g in both])
    b_swap = Group(
        b_h.at[below, :, two],
        [(b_h.at[below, g, 2], b_h.at[below, g, j], near_sem.at[halves + 2], (s, p)) for g in both for j, p in sides],
    )
    b_pass = Group(
        b_h.at[below, :, two],
        [(b_h.at[below, :, two], b_h.at[below, :, two], b_to, (HOST, q))],
    )
    lent_near = Group(
        lent.at[two],
        [
            (lent.at[0], lent.at[2], aide_sem.at[1], (AIDE, right)),
            (lent.at[1], lent.at[3], aide_sem.at[1], (AIDE, left)),
        ],
    )
    lent_back = Group(
        lent.at[two],
        [(lent.at[2 + n], z_r.at[n, high_rows], near_sem.at[halves + 1], (0, q)) for n in range(2)],
    )
    most = max(most, names.count)

    names.count = shared
    close = ((LEFT, right), (RIGHT, left))
    far = close + ((FAR_LEFT, next_right), (FAR_RIGHT, next_left))
    up_rings = range(1, top - 1, 2)

    def ring_of(kind, t):
        return halves * (t - 1) if kind == 0 else halves * (slabs - 1 + up_rings.index(t))

    def around(buf, t, kind, places):
        return Group(
            buf.at[t - 1, :, pl.ds(0, len(places))],
            [
                (buf.at[t - 1, g, OWN], buf.at[t - 1, g, j], ring_sem.at[ring_of(kind, t) + g], (s, p))
                for g in both
                for j, p in places
            ],
        )

    round_d = {t: around(d_h, t, 0, far if t == top else close) for t in range(2, slabs)}
    round_u = {t: around(u_h, t, 1, far) for t in up_rings}
    kept_c = {
        t: Group(
            b_h.at[t - 1, :, two],
            [
                (b_h.at[t - 1, g, 2], b_h.at[t - 1, g, j], term_sem.at[k_sem + t // 2], (s, p))
                for g in both
                for j, p in sides
            ],
        )
        for t in range(1, top, 2)
    }
    w_host = Group(w_h.at[0, two], [(w_h.at[0, 2], w_h.at[0, j], op_sem.at[w_sem], (s, p)) for j, p in sides])

    def back(buf, dst, recv, t):
        return Group(
            buf.at[t - 1, :, middle], [(buf.at[t - 1, g, middle], dst.at[g], recv, (t, q)) for g in both]
        )

    back_d = {t: back(d_h, d_home, home_sem.at[0], t) for t in range(2, slabs)}
    back_u = {t: back(u_h, u_home, home_sem.at[1], t) for t in range(2, top)}
    last_u = Group(u0_s, [(u0_s.at[g], u_home.at[g], home_sem.at[1 + g], (0, q)) for g in both])
    most = max(most, names.count)
    assert most == send_sem.shape[0], most

    count = margin_ref[0, 0]
    row = lax.broadcasted_iota(jnp.int32, (KMAX, KMAX), 0)
    col = lax.broadcasted_iota(jnp.int32, (KMAX, KMAX), 1)
    hit = (row == KMAX - count + col) & (col < count)
    place[...] = jnp.where(hit, 1.0, 0.0).astype(BF)

    loads[0].wait()
    loads[1].wait()
    first = solve(r_v[...].astype(BF), fac, m)
    tail_s[...] = nn(first[-1].astype(BF), place[...]).astype(BF)
    head_s[...] = first[0].astype(BF)

    pl.semaphore_wait(barrier, greeted)

    def send_tails():
        start(*tail_c)

    pl.when(first_slab)(send_tails)

    low = fac[:, :face]
    high = fac[m - face :, m - face :]
    k_tail = jnp.concatenate(
        [tn(low[m - KMAX :], fac[m - KMAX :, m - KMAX :]), tn(high, fac[m - face :, m - KMAX :])], axis=0
    )
    k_head = jnp.concatenate([tn(low, fac[:, :KMAX]), tn(high, fac[m - face :, :KMAX])], axis=0)
    zt_s[...] = nn(k_tail.astype(BF), place[...]).astype(BF)
    zh_s[...] = k_head.astype(BF)

    @pl.when(inner_low)
    def _():
        start(zd_c)

    loads[2].wait()
    loads[3].wait()
    for k, piece in enumerate(solve(maps[...], fac, m)):
        gt[:, k * KMAX : (k + 1) * KMAX] = piece.astype(BF)

    @pl.when(guest)
    def _():
        zd_c.sent()
        send_tails()

    @pl.when(first_slab)
    def _():
        tail_c[0].sent()
        pl.semaphore_signal(turn_sem, inc=1, device_id=(HOST, q), device_id_type=MESH)

    @pl.when(host)
    def _():
        pl.semaphore_wait(turn_sem, 1)
        send_tails()

    @pl.when(inner_low)
    def _():
        arrived(z_r.at[:, low_rows], near_sem.at[halves])
        zr[low_rows] = nt(z_r[1, low_rows], place[...]).astype(BF)
        own = (-gt[:, :face].astype(F32)).T.astype(BF)
        from_left = (0.5 * nt(z_r[0, low_rows], gt[:, :KMAX])).astype(BF)
        from_right = (0.5 * nt(zr[low_rows], gt[:, m - KMAX :])).astype(BF)
        for n, block in enumerate((own, from_left, from_right)):
            lines = pl.ds(n * face, face)
            t_h[below, lines] = block[:, :face]

            @pl.when(inner_high)
            def _():
                v_h[below, lines] = block[:, face:]

            @pl.when(~inner_high)
            def _():
                w_h[below, 2, lines] = block[:, face:]

        @pl.when(guest & inner_high)
        def _():
            start(t_c, v_c)

        @pl.when(last)
        def _():
            start(w_c)

    for g, w in enumerate(part):
        arrived(side_r.at[:, w], near_sem.at[g])
        adj[w, :] = r_v[w, :]
        adj[w, :KMAX] = adj[w, :KMAX] - 0.5 * side_r[0, w].astype(F32)
        adj[w, m - KMAX :] = adj[w, m - KMAX :] - 0.5 * nt(side_r[1, w], place[...])

        @pl.when(first_slab)
        def _():
            d_s[w] = nt(adj[w, :].astype(BF), gt[:face]).astype(BF)
            seed_c.start(3 * g, 3 * g + 3)

        @pl.when(inner_low)
        def _():
            terms = nt(adj[w, :].astype(BF), gt[...]).astype(BF)
            a_h[below, g] = terms[:, :face]
            b_h[below, g, 2] = terms[:, face:]

            @pl.when(guest & inner_high)
            def _():
                a_c.start(g, g + 1)
                if g == 0:
                    start(zu_c)

            @pl.when(guest)
            def _():
                b_c.start(g, g + 1)

            @pl.when(last)
            def _():
                b_swap.start(2 * g, 2 * g + 2)

    @pl.when(last)
    def _():
        start(w_near)
        arrived(b_h.at[below, :, two], near_sem.at[halves + 2])
        start(b_pass)

    @pl.when(first_slab)
    def _():
        start(lent_c)

    def make_up():
        arrived(z_r.at[:, high_rows], near_sem.at[halves + 1])
        zr[high_rows] = nt(z_r[1, high_rows], place[...]).astype(BF)

        @pl.when(inner_low)
        def _():
            w_h[below, 2, :face] = (-gt[face:, m - face :].astype(F32)).T.astype(BF)
            w_h[below, 2, face : 2 * face] = (0.5 * nt(z_r[0, high_rows], gt[face:, :KMAX])).astype(BF)
            w_h[below, 2, 2 * face :] = (0.5 * nt(zr[high_rows], gt[face:, m - KMAX :])).astype(BF)

    @pl.when(guest & inner_high)
    def _():
        make_up()
        start(w_c)

        @pl.when(odd)
        def _():
            start(w_near)

    @pl.when(aide)
    def _():
        arrived(lent.at[two], aide_sem.at[0])
        start(lent_near)
        arrived(lent.at[pl.ds(2, 2)], aide_sem.at[1])
        start(lent_back)

    def beside(ref, n, g, slots):
        return jnp.concatenate([ref[n, g, j] for j in slots], axis=1)

    centre = (OWN, LEFT, RIGHT)

    @pl.when(host)
    def _():
        for t in range(1, top):
            n = t - 1
            if t > HOST:
                arrived(t_h.at[n], op_sem.at[t_sem + n - 1])
            for g in both:
                if t > HOST:
                    arrived(a_h.at[n, g], term_sem.at[a_sem + halves * (n - 1) + g])
                arrived(d_h.at[n, g, pl.ds(2, 3 if t == 1 else 2)], ring_sem.at[ring_of(0, t) + g])
                d_h[n + 1, g, OWN] = (a_h[n, g].astype(F32) + nn(beside(d_h, n, g, centre), t_h[n])).astype(BF)
                per = len(far if t + 1 == top else close)
                round_d[t + 1].start(per * g, per * g + per)
            if t == 1:
                start(zu_c)
            if t > HOST:
                back_d[t].start()
                if t % 2 == 0:
                    kept_c[t - 1].start()
                arrived(v_h.at[n], op_sem.at[v_sem + n - 1])
                arrived(b_h.at[n, :, 2], term_sem.at[b_sem + n - 1])
            for g in both:
                b_h[n, g, 2] = (b_h[n, g, 2].astype(F32) + nn(beside(d_h, n, g, centre), v_h[n])).astype(BF)
            if t == min(2, top - 1):
                make_up()
                start(w_host)

        arrived(w_h.at[top - 1], op_sem.at[w_sem + top - 1])
        for t in range(top, 0, -2):
            n = t - 1
            state = d_h if t == top else u_h
            if t < top:
                arrived(w_h.at[n, two] if t == HOST else w_h.at[n], op_sem.at[w_sem + n])
            if t > 1:
                arrived(w_h.at[n - 1, 2], op_sem.at[w_sem + n - 1])
            if t == top:
                arrived(b_h.at[n], term_sem.at[b_sem + n - 1])
            else:
                arrived(b_h.at[n, :, two], term_sem.at[k_sem + t // 2])
            for g in both:
                arrived(state.at[n, g, four], ring_sem.at[ring_of(0 if t == top else 1, t) + g])
                for j, slots in enumerate(((LEFT, FAR_LEFT, OWN), (RIGHT, OWN, FAR_RIGHT), centre)):
                    u = (b_h[n, g, j].astype(F32) + nn(beside(state, n, g, slots), w_h[n, j])).astype(BF)
                    if t > 1:
                        u_h[n - 1, g, 2 + j] = u
                    else:
                        u0_s[g, j] = u
                if t > 1:
                    u = b_h[n - 1, g, 2].astype(F32) + nn(beside(u_h, n - 1, g, centre), w_h[n - 1, 2])
                    u_h[n - 2, g, OWN] = u.astype(BF)
                    round_u[t - 2].start(4 * g, 4 * g + 4)
                    back_u[t - 1].start(g, g + 1)
                else:
                    last_u.start(g, g + 1)
                if t > HOST:
                    (back_d if t == top else back_u)[t].start(g, g + 1)

    def drop_low(get):
        for g, w in enumerate(part):
            adj[w, :face] = adj[w, :face] - get(g, 2).astype(F32)
            adj[w, :KMAX] = adj[w, :KMAX] + 0.5 * nn(get(g, 0), z_r[0, low_rows])
            adj[w, m - KMAX :] = adj[w, m - KMAX :] + 0.5 * nn(get(g, 1), zr[low_rows])

    def drop_high(g, get):
        w = part[g]
        adj[w, m - face :] = adj[w, m - face :] - get(g, 2).astype(F32)
        adj[w, :KMAX] = adj[w, :KMAX] + 0.5 * nn(get(g, 0), z_r[0, high_rows])
        adj[w, m - KMAX :] = adj[w, m - KMAX :] + 0.5 * nn(get(g, 1), zr[high_rows])

    @pl.when(host)
    def _():
        drop_low(lambda g, j: d_h[0, g, 2 + j])
        if HOST < top:
            for g in both:
                drop_high(g, lambda g, j: u_h[0, g, 2 + j])

    @pl.when(guest)
    def _():
        arrived(d_home, home_sem.at[0])
        drop_low(lambda g, j: d_home[g, j])

    @pl.when(guest & inner_high)
    def _():
        arrived(u_home, home_sem.at[1])
        for g in both:
            drop_high(g, lambda g, j: u_home[g, j])

    @pl.when(first_slab)
    def _():
        make_up()
        for g in both:
            arrived(u_home.at[g], home_sem.at[1 + g])
            drop_high(g, lambda g, j: u_home[g, j])

    for k, piece in enumerate(solve(adj[...].astype(BF), fac, m)):
        out_ref[0, 0, :, k * KMAX : (k + 1) * KMAX] = piece

    @pl.when(first_slab)
    def _():
        sent(tail_c[1], lent_c, seed_c)

    @pl.when(inner_low)
    def _():
        sent(tail_c[1])

    @pl.when(host)
    def _():
        sent(zd_c, tail_c[0])

    @pl.when(guest)
    def _():
        sent(tail_c[0])

    @pl.when(inner_low & inner_high)
    def _():
        sent(zu_c)

    @pl.when(aide)
    def _():
        sent(lent_near, lent_back)

    @pl.when(guest)
    def _():
        sent(w_c, b_c)

    @pl.when(guest & inner_high)
    def _():
        sent(t_c, v_c, a_c)

    @pl.when(odd_guest)
    def _():
        sent(w_near)

    @pl.when(last)
    def _():
        sent(b_swap, b_pass)

    @pl.when(host)
    def _():
        sent(w_host, last_u)
        for kind in (round_d, round_u, kept_c, back_d, back_u):
            sent(*kind.values())


def on_device(slabs, patches, right_side, inverse_factor, forward_trace, backward_trace, margin):
    cols, m = right_side.shape[2:]
    face = forward_trace.shape[2]
    halves = 2
    rows = cols // halves
    links = slabs - 1
    wide = pltpu.VMEM((cols, KMAX), BF)
    square = pltpu.VMEM((2 * face, KMAX), BF)
    hbm = pl.BlockSpec(memory_space=pltpu.HBM)
    home = pltpu.VMEM((halves, 3, rows, face), BF)
    ops = pltpu.VMEM((links, 3 * face, face), BF)
    ring = pltpu.VMEM((links, halves, 5, rows, face), BF)
    sends = halves + 2 + max(10, 2 * (links - 1) + (links - 2) + 3 * (slabs // 2 - 1) - (slabs // 2 - 1) + 2)
    return pl.pallas_call(
        functools.partial(kernel, slabs, patches, halves),
        out_shape=pltpu.VMEM(right_side.shape, F32),
        in_specs=[hbm, hbm, hbm, hbm, pl.BlockSpec(memory_space=pltpu.SMEM)],
        out_specs=pl.BlockSpec(memory_space=pltpu.VMEM),
        scratch_shapes=[
            pltpu.VMEM((cols, m), F32),
            pltpu.VMEM((m, m), BF),
            pltpu.VMEM((2 * face, m), BF),
            wide, wide, square, square, pltpu.VMEM((cols, face), BF),
            pltpu.VMEM((2, cols, KMAX), BF), pltpu.VMEM((2, 2 * face, KMAX), BF), home, home,
            pltpu.VMEM((links, halves, rows, face), BF),
            pltpu.VMEM((links, halves, 3, rows, face), BF),
            ops, ops, pltpu.VMEM((links, 3, 3 * face, face), BF),
            ring, ring, home,
            pltpu.VMEM((cols, m), F32),
            pltpu.VMEM((2 * face, m), BF),
            pltpu.VMEM((KMAX, KMAX), BF),
            square,
            pltpu.VMEM((4, face, KMAX), BF),
            pltpu.SemaphoreType.DMA((4,)),
            pltpu.SemaphoreType.DMA((sends,)),
            pltpu.SemaphoreType.DMA((halves + 3,)),
            pltpu.SemaphoreType.DMA((1 + halves,)),
            pltpu.SemaphoreType.DMA((2 * (links - 2) + links,)),
            pltpu.SemaphoreType.DMA((halves * (links - 2) + links - 1 + slabs // 2 - 1,)),
            pltpu.SemaphoreType.DMA((halves * (links + slabs // 2 - 1),)),
            pltpu.SemaphoreType.DMA((2,)),
            pltpu.SemaphoreType.REGULAR,
        ],
        compiler_params=pltpu.CompilerParams(collective_id=0, has_side_effects=True),
        name="sweeps",
    )(right_side, inverse_factor, forward_trace, backward_trace, margin)
    return pl.pallas_call(
        finish,
        out_shape=jax.ShapeDtypeStruct(right_side.shape, F32),
        in_specs=[pl.BlockSpec(memory_space=pltpu.VMEM)] * 2,
        out_specs=hbm,
        scratch_shapes=[pltpu.VMEM((m // KMAX, cols, KMAX), F32), pltpu.SemaphoreType.DMA((m // KMAX,))],
        compiler_params=pltpu.CompilerParams(vmem_limit_bytes=16 << 20),
        name="finish",
    )(half, inverse_factor)


def solution(mesh):
    four = P("slab", "patch", None, None)
    return jax.shard_map(
        functools.partial(on_device, mesh.shape["slab"], mesh.shape["patch"]),
        mesh=mesh,
        in_specs=(four, four, four, four, P("slab", "patch")),
        out_specs=four,
        check_vma=False,
    )
```

```python
import functools

import jax
import jax.numpy as jnp
from jax import lax
from jax.experimental import pallas as pl
from jax.experimental.pallas import tpu as pltpu
from jax.sharding import PartitionSpec as P

KMAX = 256
BF = jnp.bfloat16
F32 = jnp.float32
MESH = pl.DeviceIdType.MESH


def nt(a, b):
    return lax.dot_general(a, b, (((1,), (1,)), ((), ())), preferred_element_type=F32)


def nn(a, b):
    return lax.dot_general(a, b, (((1,), (0,)), ((), ())), preferred_element_type=F32)


def tn(a, b):
    return lax.dot_general(a, b, (((0,), (0,)), ((), ())), preferred_element_type=F32)


def halfway(x, fac, m):
    return jnp.concatenate(
        [nt(x[:, : i + KMAX], fac[i : i + KMAX, : i + KMAX]).astype(BF) for i in range(0, m, KMAX)],
        axis=1,
    )


def solve(x, fac, m):
    half = halfway(x, fac, m)
    return [nn(half[:, k:], fac[k:, k : k + KMAX]) for k in range(0, m, KMAX)]


def finish(half_ref, l_ref, out_ref, held, sem):
    m = half_ref.shape[1]
    copies = []
    for n, k in enumerate(range(0, m, KMAX)):
        held[n] = nn(half_ref[:, k:], l_ref[0, 0, k:, k : k + KMAX])
        copies.append(pltpu.make_async_copy(held.at[n], out_ref.at[0, 0, :, k : k + KMAX], sem.at[n]))
        copies[-1].start()
    for c in copies:
        c.wait()


FAR_LEFT, FAR_RIGHT, LEFT, RIGHT, OWN = range(5)
HOST, AIDE = 1, 2


class Names:
    def __init__(self):
        self.count = 0

    def take(self):
        self.count += 1
        return self.count - 1


def kernel(
    slabs, patches, halves,
    r_hbm, l_hbm, f_hbm, b_hbm, margin_ref, out_ref,
    r_v, fac, maps,
    tail_s, head_s, zt_s, zh_s, d_s,
    side_r, z_r, d_home, u_home,
    a_h, b_h, t_h, v_h, w_h, d_h, u_h, u0_s,
    adj, gt, place, zr, lent, effect,
    load_sem, send_sem, near_sem, home_sem, op_sem, term_sem, ring_sem, aide_sem, turn_sem,
):
    s = lax.axis_index("slab")
    q = lax.axis_index("patch")
    left = lax.rem(q + patches - 1, patches)
    right = lax.rem(q + 1, patches)
    next_left = lax.rem(q + patches - 2, patches)
    next_right = lax.rem(q + 2, patches)
    pair = s + 1 - 2 * lax.rem(s, 2)
    odd = lax.rem(s, 2) == 1
    m = fac.shape[-1]
    face = f_hbm.shape[-2]
    cols = r_v.shape[0]
    top = slabs - 1
    wide = cols // halves
    inner_low, inner_high = s > 0, s < top
    first_slab = s == 0
    host, guest, last = s == HOST, s > HOST, s == top
    odd_guest = guest & odd
    aide = s == AIDE

    loads = [
        pltpu.make_async_copy(l_hbm.at[0, 0], fac, load_sem.at[1]),
        pltpu.make_async_copy(r_hbm.at[0, 0], r_v, load_sem.at[0]),
        pltpu.make_async_copy(f_hbm.at[0, 0], maps.at[:face], load_sem.at[2]),
        pltpu.make_async_copy(b_hbm.at[0, 0], maps.at[face:], load_sem.at[3]),
    ]
    for c in loads:
        c.start()

    barrier = pltpu.get_barrier_semaphore()

    def greet(slab, patch):
        pl.semaphore_signal(barrier, inc=1, device_id=(slab, patch), device_id_type=MESH)

    greet(s, left)
    greet(s, right)
    greet(pair, q)

    @pl.when(first_slab)
    def _():
        greet(HOST, left)
        greet(HOST, right)
        greet(AIDE, q)

    @pl.when(aide)
    def _():
        greet(0, q)

    @pl.when(guest)
    def _():
        greet(HOST, q)

    @pl.when(odd_guest)
    def _():
        greet(HOST, left)
        greet(HOST, right)

    @pl.when(host)
    def _():
        greet(s, next_left)
        greet(s, next_right)
        greet(0, left)
        greet(0, right)
        for t in range(HOST + 1, slabs):
            greet(t, q)
        for t in range(HOST + 2, slabs, 2):
            greet(t, left)
            greet(t, right)

    greeted = (
        3
        + first_slab.astype(jnp.int32) * 3
        + aide.astype(jnp.int32)
        + guest.astype(jnp.int32)
        + odd_guest.astype(jnp.int32) * 2
        + host.astype(jnp.int32) * (4 + slabs - 2 + 2 * len(range(HOST + 2, slabs, 2)))
    )

    names = Names()

    class Group:
        def __init__(self, whole, copies):
            self.whole, self.sem = whole, send_sem.at[names.take()]
            self.copies = [
                pltpu.make_async_remote_copy(
                    src_ref=src, dst_ref=dst, send_sem=self.sem, recv_sem=recv, device_id=place, device_id_type=MESH
                )
                for src, dst, recv, place in copies
            ]

        def start(self, first=0, end=None):
            for c in self.copies[first:end]:
                c.start()

        def sent(self):
            arrived(self.whole, self.sem)

    def arrived(ref, sem):
        pltpu.make_async_copy(ref, ref, sem).wait()

    def start(*groups):
        for c in groups:
            c.start()

    def sent(*groups):
        for c in groups:
            c.sent()

    part = [pl.ds(g * wide, wide) for g in range(halves)]
    both = range(halves)
    low_rows, high_rows = pl.ds(0, face), pl.ds(face, face)
    two, four, middle = pl.ds(0, 2), pl.ds(0, 4), pl.ds(2, 3)

    tail_c = [
        Group(
            tail_s,
            [
                (tail_s.at[w], side_r.at[0, w], near_sem.at[g], (s, right)),
                (head_s.at[w], side_r.at[1, w], near_sem.at[g], (s, left)),
            ],
        )
        for g, w in enumerate(part)
    ]

    def z_rows(rows, n):
        return Group(
            zt_s,
            [
                (zt_s.at[rows], z_r.at[0, rows], near_sem.at[halves + n], (s, right)),
                (zh_s.at[rows], z_r.at[1, rows], near_sem.at[halves + n], (s, left)),
            ],
        )

    zd_c, zu_c = z_rows(low_rows, 0), z_rows(high_rows, 1)
    shared = names.count

    seed_c = Group(
        d_h.at[0, :, middle],
        [
            (d_s.at[w], d_h.at[0, g, j], ring_sem.at[g], (HOST, p))
            for g, w in enumerate(part)
            for j, p in ((LEFT, right), (RIGHT, left), (OWN, q))
        ],
    )
    lent_c = Group(
        zt_s,
        [
            (zt_s.at[high_rows], lent.at[0], aide_sem.at[0], (AIDE, q)),
            (zh_s.at[high_rows], lent.at[1], aide_sem.at[0], (AIDE, q)),
        ],
    )
    most = names.count

    names.count = shared
    below = jnp.maximum(s - 1, 0)
    inner = jnp.maximum(s - 2, 0)
    inners = slabs - 3
    sides = ((0, right), (1, left))
    t_sem, v_sem, w_sem = 0, inners, 2 * inners
    a_sem, b_sem, k_sem = 0, halves * inners, halves * inners + slabs - 2
    t_c = Group(t_h.at[below], [(t_h.at[below], t_h.at[below], op_sem.at[t_sem + inner], (HOST, q))])
    v_c = Group(v_h.at[below], [(v_h.at[below], v_h.at[below], op_sem.at[v_sem + inner], (HOST, q))])
    w_to = op_sem.at[w_sem + below]
    w_c = Group(w_h.at[below, 2], [(w_h.at[below, 2], w_h.at[below, 2], w_to, (HOST, q))])
    w_near = Group(w_h.at[below, two], [(w_h.at[below, 2], w_h.at[below, j], w_to, (HOST, p)) for j, p in sides])
    a_c = Group(
        a_h.at[below],
        [(a_h.at[below, g], a_h.at[below, g], term_sem.at[a_sem + halves * inner + g], (HOST, q)) for g in both],
    )
    b_to = term_sem.at[b_sem + inner]
    b_c = Group(b_h.at[below, :, 2], [(b_h.at[below, g, 2], b_h.at[below, g, 2], b_to, (HOST, q)) for g in both])
    b_swap = Group(
        b_h.at[below, :, two],
        [(b_h.at[below, g, 2], b_h.at[below, g, j], near_sem.at[halves + 2], (s, p)) for g in both for j, p in sides],
    )
    b_pass = Group(
        b_h.at[below, :, two],
        [(b_h.at[below, :, two], b_h.at[below, :, two], b_to, (HOST, q))],
    )
    lent_near = Group(
        lent.at[two],
        [
            (lent.at[0], lent.at[2], aide_sem.at[1], (AIDE, right)),
            (lent.at[1], lent.at[3], aide_sem.at[2], (AIDE, left)),
        ],
    )
    lent_back = Group(
        lent.at[two],
        [(lent.at[2 + n], z_r.at[n, high_rows], near_sem.at[halves + 1], (0, q)) for n in range(2)],
    )
    most = max(most, names.count)

    names.count = shared
    close = ((LEFT, right), (RIGHT, left))
    far = close + ((FAR_LEFT, next_right), (FAR_RIGHT, next_left))
    up_rings = range(1, top - 1, 2)

    def ring_of(kind, t):
        return halves * (t - 1) if kind == 0 else halves * (slabs - 1 + up_rings.index(t))

    def around(buf, t, kind, places):
        return Group(
            buf.at[t - 1, :, pl.ds(0, len(places))],
            [
                (buf.at[t - 1, g, OWN], buf.at[t - 1, g, j], ring_sem.at[ring_of(kind, t) + g], (s, p))
                for g in both
                for j, p in places
            ],
        )

    round_d = {t: around(d_h, t, 0, far if t == top else close) for t in range(2, slabs)}
    round_u = {t: around(u_h, t, 1, far) for t in up_rings}
    kept_c = {
        t: Group(
            b_h.at[t - 1, :, two],
            [
                (b_h.at[t - 1, g, 2], b_h.at[t - 1, g, j], term_sem.at[k_sem + t // 2], (s, p))
                for g in both
                for j, p in sides
            ],
        )
        for t in range(1, top, 2)
    }
    w_host = Group(w_h.at[0, two], [(w_h.at[0, 2], w_h.at[0, j], op_sem.at[w_sem], (s, p)) for j, p in sides])

    def back(buf, dst, recv, t):
        return Group(
            buf.at[t - 1, :, middle], [(buf.at[t - 1, g, middle], dst.at[g], recv, (t, q)) for g in both]
        )

    back_d = {t: back(d_h, d_home, home_sem.at[0], t) for t in range(2, slabs)}
    back_u = {t: back(u_h, u_home, home_sem.at[1], t) for t in range(2, top)}
    last_u = Group(u0_s, [(u0_s.at[g], u_home.at[g], home_sem.at[1 + g], (0, q)) for g in both])
    most = max(most, names.count)
    assert most == send_sem.shape[0], most

    count = margin_ref[0, 0]
    row = lax.broadcasted_iota(jnp.int32, (KMAX, KMAX), 0)
    col = lax.broadcasted_iota(jnp.int32, (KMAX, KMAX), 1)
    hit = (row == KMAX - count + col) & (col < count)
    place[...] = jnp.where(hit, 1.0, 0.0).astype(BF)

    loads[0].wait()
    loads[1].wait()
    first = solve(r_v[...].astype(BF), fac, m)
    tail_s[...] = nn(first[-1].astype(BF), place[...]).astype(BF)
    head_s[...] = first[0].astype(BF)

    pl.semaphore_wait(barrier, greeted)

    def send_tails():
        start(*tail_c)

    pl.when(first_slab)(send_tails)

    low = fac[:, :face]
    high = fac[m - face :, m - face :]
    k_tail = jnp.concatenate(
        [tn(low[m - KMAX :], fac[m - KMAX :, m - KMAX :]), tn(high, fac[m - face :, m - KMAX :])], axis=0
    )
    k_head = jnp.concatenate([tn(low, fac[:, :KMAX]), tn(high, fac[m - face :, :KMAX])], axis=0)
    zt_s[...] = nn(k_tail.astype(BF), place[...]).astype(BF)
    zh_s[...] = k_head.astype(BF)

    far_right, far_left = q == patches - 1, q == 0

    def lift_far():
        @pl.when(far_right)
        def _():
            zu_c.start(0, 1)

        @pl.when(far_left)
        def _():
            zu_c.start(1, 2)

    def lift():
        @pl.when(~far_right)
        def _():
            zu_c.start(0, 1)

        @pl.when(~far_left)
        def _():
            zu_c.start(1, 2)

    @pl.when(inner_low)
    def _():
        start(zd_c)

    pl.when(guest & inner_high)(lift_far)

    loads[2].wait()
    loads[3].wait()
    for k, piece in enumerate(solve(maps[...], fac, m)):
        gt[:, k * KMAX : (k + 1) * KMAX] = piece.astype(BF)

    @pl.when(guest)
    def _():
        zd_c.sent()
        send_tails()

    @pl.when(first_slab)
    def _():
        tail_c[0].sent()
        pl.semaphore_signal(turn_sem, inc=1, device_id=(HOST, q), device_id_type=MESH)

    @pl.when(host)
    def _():
        pl.semaphore_wait(turn_sem, 1)
        send_tails()

    @pl.when(inner_low)
    def _():
        arrived(z_r.at[:, low_rows], near_sem.at[halves])
        zr[low_rows] = nt(z_r[1, low_rows], place[...]).astype(BF)
        own = (-gt[:, :face].astype(F32)).T.astype(BF)
        from_left = (0.5 * nt(z_r[0, low_rows], gt[:, :KMAX])).astype(BF)
        from_right = (0.5 * nt(zr[low_rows], gt[:, m - KMAX :])).astype(BF)
        for n, block in enumerate((own, from_left, from_right)):
            lines = pl.ds(n * face, face)
            t_h[below, lines] = block[:, :face]

            @pl.when(inner_high)
            def _():
                v_h[below, lines] = block[:, face:]

            @pl.when(~inner_high)
            def _():
                w_h[below, 2, lines] = block[:, face:]

        @pl.when(guest & inner_high)
        def _():
            start(t_c, v_c)

        @pl.when(last)
        def _():
            start(w_c)

    for g, w in enumerate(part):
        arrived(side_r.at[:, w], near_sem.at[g])
        adj[w, :] = r_v[w, :]
        adj[w, :KMAX] = adj[w, :KMAX] - 0.5 * side_r[0, w].astype(F32)
        adj[w, m - KMAX :] = adj[w, m - KMAX :] - 0.5 * nt(side_r[1, w], place[...])

        @pl.when(first_slab)
        def _():
            d_s[w] = nt(adj[w, :].astype(BF), gt[:face]).astype(BF)
            seed_c.start(3 * g, 3 * g + 3)

        @pl.when(inner_low)
        def _():
            terms = nt(adj[w, :].astype(BF), gt[...]).astype(BF)
            a_h[below, g] = terms[:, :face]
            b_h[below, g, 2] = terms[:, face:]

            @pl.when(guest & inner_high)
            def _():
                a_c.start(g, g + 1)
                if g == 0:
                    lift()

            @pl.when(guest)
            def _():
                b_c.start(g, g + 1)

            @pl.when(last)
            def _():
                b_swap.start(2 * g, 2 * g + 2)

    @pl.when(last)
    def _():
        start(w_near)
        arrived(b_h.at[below, :, two], near_sem.at[halves + 2])
        start(b_pass)

    @pl.when(first_slab)
    def _():
        start(lent_c)
        for k, piece in enumerate(solve(adj[...].astype(BF), fac, m)):
            out_ref[0, 0, :, k * KMAX : (k + 1) * KMAX] = piece
        effect[:face] = (-tn(fac[m - face :, m - face :], fac[m - face :, :])).astype(BF)

    def make_up():
        arrived(z_r.at[:, high_rows], near_sem.at[halves + 1])
        zr[high_rows] = nt(z_r[1, high_rows], place[...]).astype(BF)

        @pl.when(inner_low)
        def _():
            w_h[below, 2, :face] = (-gt[face:, m - face :].astype(F32)).T.astype(BF)
            w_h[below, 2, face : 2 * face] = (0.5 * nt(z_r[0, high_rows], gt[face:, :KMAX])).astype(BF)
            w_h[below, 2, 2 * face :] = (0.5 * nt(zr[high_rows], gt[face:, m - KMAX :])).astype(BF)

    @pl.when(guest & inner_high)
    def _():
        make_up()
        start(w_c)

        @pl.when(odd)
        def _():
            start(w_near)

    @pl.when(aide)
    def _():
        arrived(lent.at[two], aide_sem.at[0])
        start(lent_near)

        @pl.when(q == 0)
        def _():
            arrived(lent.at[3], aide_sem.at[2])
            lent_back.start(1, 2)
            arrived(lent.at[2], aide_sem.at[1])
            lent_back.start(0, 1)

        @pl.when(q > 0)
        def _():
            arrived(lent.at[2], aide_sem.at[1])
            lent_back.start(0, 1)
            arrived(lent.at[3], aide_sem.at[2])
            lent_back.start(1, 2)

    def beside(ref, n, g, slots):
        return jnp.concatenate([ref[n, g, j] for j in slots], axis=1)

    centre = (OWN, LEFT, RIGHT)

    def drop_low(get):
        for g, w in enumerate(part):
            adj[w, :face] = adj[w, :face] - get(g, 2).astype(F32)
            adj[w, :KMAX] = adj[w, :KMAX] + 0.5 * nn(get(g, 0), z_r[0, low_rows])
            adj[w, m - KMAX :] = adj[w, m - KMAX :] + 0.5 * nn(get(g, 1), zr[low_rows])

    def drop_high(g, get):
        w = part[g]
        adj[w, m - face :] = adj[w, m - face :] - get(g, 2).astype(F32)
        adj[w, :KMAX] = adj[w, :KMAX] + 0.5 * nn(get(g, 0), z_r[0, high_rows])
        adj[w, m - KMAX :] = adj[w, m - KMAX :] + 0.5 * nn(get(g, 1), zr[high_rows])

    @pl.when(host)
    def _():
        for t in range(1, top):
            n = t - 1
            if t > HOST:
                arrived(t_h.at[n], op_sem.at[t_sem + n - 1])
            for g in both:
                if t > HOST:
                    arrived(a_h.at[n, g], term_sem.at[a_sem + halves * (n - 1) + g])
                arrived(d_h.at[n, g, pl.ds(2, 3 if t == 1 else 2)], ring_sem.at[ring_of(0, t) + g])
                d_h[n + 1, g, OWN] = (a_h[n, g].astype(F32) + nn(beside(d_h, n, g, centre), t_h[n])).astype(BF)
                per = len(far if t + 1 == top else close)
                round_d[t + 1].start(per * g, per * g + per)
            if t == 1:
                start(zu_c)
            if t > HOST:
                back_d[t].start()
                if t % 2 == 0:
                    kept_c[t - 1].start()
                arrived(v_h.at[n], op_sem.at[v_sem + n - 1])
                arrived(b_h.at[n, :, 2], term_sem.at[b_sem + n - 1])
            for g in both:
                b_h[n, g, 2] = (b_h[n, g, 2].astype(F32) + nn(beside(d_h, n, g, centre), v_h[n])).astype(BF)
            if t == min(2, top - 1):
                make_up()
                start(w_host)

        drop_low(lambda g, j: d_h[0, g, 2 + j])
        arrived(w_h.at[top - 1], op_sem.at[w_sem + top - 1])
        for t in range(top, 0, -2):
            n = t - 1
            state = d_h if t == top else u_h
            if t < top:
                arrived(w_h.at[n, two] if t == HOST else w_h.at[n], op_sem.at[w_sem + n])
            if t > 1:
                arrived(w_h.at[n - 1, 2], op_sem.at[w_sem + n - 1])
            if t == top:
                arrived(b_h.at[n], term_sem.at[b_sem + n - 1])
            else:
                arrived(b_h.at[n, :, two], term_sem.at[k_sem + t // 2])
            for g in both:
                arrived(state.at[n, g, four], ring_sem.at[ring_of(0 if t == top else 1, t) + g])
                for j, slots in enumerate(((LEFT, FAR_LEFT, OWN), (RIGHT, OWN, FAR_RIGHT), centre)):
                    u = (b_h[n, g, j].astype(F32) + nn(beside(state, n, g, slots), w_h[n, j])).astype(BF)
                    if t > 1:
                        u_h[n - 1, g, 2 + j] = u
                    else:
                        u0_s[g, j] = u
                if t > 1:
                    u = b_h[n - 1, g, 2].astype(F32) + nn(beside(u_h, n - 1, g, centre), w_h[n - 1, 2])
                    u_h[n - 2, g, OWN] = u.astype(BF)
                    round_u[t - 2].start(4 * g, 4 * g + 4)
                    back_u[t - 1].start(g, g + 1)
                else:
                    last_u.start(g, g + 1)
                if t > HOST:
                    (back_d if t == top else back_u)[t].start(g, g + 1)

    @pl.when(host)
    def _():
        if HOST < top:
            for g in both:
                drop_high(g, lambda g, j: u_h[0, g, 2 + j])

    @pl.when(guest)
    def _():
        arrived(d_home, home_sem.at[0])
        drop_low(lambda g, j: d_home[g, j])

    @pl.when(guest & inner_high)
    def _():
        arrived(u_home, home_sem.at[1])
        for g in both:
            drop_high(g, lambda g, j: u_home[g, j])

    @pl.when(first_slab)
    def _():
        arrived(z_r.at[:, high_rows], near_sem.at[halves + 1])
        half = jnp.concatenate(
            [nt(z_r[0, high_rows], fac[i : i + KMAX, :KMAX]).astype(BF) for i in range(0, m, KMAX)], axis=1
        )
        for k in range(0, m, KMAX):
            spread = 0.5 * nn(half[:, k:], fac[k:, k : k + KMAX])
            effect[face : 2 * face, k : k + KMAX] = spread.astype(BF)
        at_tail = nt(z_r[1, high_rows], place[...]).astype(BF)
        half = nt(at_tail, fac[m - KMAX :, m - KMAX :]).astype(BF)
        effect[2 * face :] = (0.5 * nn(half, fac[m - KMAX :, :])).astype(BF)
        for g, w in enumerate(part):
            arrived(u_home.at[g], home_sem.at[1 + g])
            u = jnp.concatenate([u_home[g, j] for j in (2, 0, 1)], axis=1)
            out_ref[0, 0, w, :] = out_ref[0, 0, w, :] + nn(u, effect[...])

    @pl.when(inner_low)
    def _():
        for k, piece in enumerate(solve(adj[...].astype(BF), fac, m)):
            out_ref[0, 0, :, k * KMAX : (k + 1) * KMAX] = piece

    @pl.when(first_slab)
    def _():
        sent(tail_c[1], lent_c, seed_c)

    @pl.when(inner_low)
    def _():
        sent(tail_c[1])

    @pl.when(host)
    def _():
        sent(zd_c, tail_c[0])

    @pl.when(guest)
    def _():
        sent(tail_c[0])

    @pl.when(inner_low & inner_high)
    def _():
        sent(zu_c)

    @pl.when(aide)
    def _():
        sent(lent_near, lent_back)

    @pl.when(guest)
    def _():
        sent(w_c, b_c)

    @pl.when(guest & inner_high)
    def _():
        sent(t_c, v_c, a_c)

    @pl.when(odd_guest)
    def _():
        sent(w_near)

    @pl.when(last)
    def _():
        sent(b_swap, b_pass)

    @pl.when(host)
    def _():
        sent(w_host, last_u)
        for kind in (round_d, round_u, kept_c, back_d, back_u):
            sent(*kind.values())


def on_device(slabs, patches, right_side, inverse_factor, forward_trace, backward_trace, margin):
    cols, m = right_side.shape[2:]
    face = forward_trace.shape[2]
    halves = 2
    rows = cols // halves
    links = slabs - 1
    wide = pltpu.VMEM((cols, KMAX), BF)
    square = pltpu.VMEM((2 * face, KMAX), BF)
    hbm = pl.BlockSpec(memory_space=pltpu.HBM)
    home = pltpu.VMEM((halves, 3, rows, face), BF)
    ops = pltpu.VMEM((links, 3 * face, face), BF)
    ring = pltpu.VMEM((links, halves, 5, rows, face), BF)
    sends = halves + 2 + max(10, 2 * (links - 1) + (links - 2) + 3 * (slabs // 2 - 1) - (slabs // 2 - 1) + 2)
    return pl.pallas_call(
        functools.partial(kernel, slabs, patches, halves),
        out_shape=pltpu.VMEM(right_side.shape, F32),
        in_specs=[hbm, hbm, hbm, hbm, pl.BlockSpec(memory_space=pltpu.SMEM)],
        out_specs=pl.BlockSpec(memory_space=pltpu.VMEM),
        scratch_shapes=[
            pltpu.VMEM((cols, m), F32),
            pltpu.VMEM((m, m), BF),
            pltpu.VMEM((2 * face, m), BF),
            wide, wide, square, square, pltpu.VMEM((cols, face), BF),
            pltpu.VMEM((2, cols, KMAX), BF), pltpu.VMEM((2, 2 * face, KMAX), BF), home, home,
            pltpu.VMEM((links, halves, rows, face), BF),
            pltpu.VMEM((links, halves, 3, rows, face), BF),
            ops, ops, pltpu.VMEM((links, 3, 3 * face, face), BF),
            ring, ring, home,
            pltpu.VMEM((cols, m), F32),
            pltpu.VMEM((2 * face, m), BF),
            pltpu.VMEM((KMAX, KMAX), BF),
            square,
            pltpu.VMEM((4, face, KMAX), BF),
            pltpu.VMEM((3 * face, m), BF),
            pltpu.SemaphoreType.DMA((4,)),
            pltpu.SemaphoreType.DMA((sends,)),
            pltpu.SemaphoreType.DMA((halves + 3,)),
            pltpu.SemaphoreType.DMA((1 + halves,)),
            pltpu.SemaphoreType.DMA((2 * (links - 2) + links,)),
            pltpu.SemaphoreType.DMA((halves * (links - 2) + links - 1 + slabs // 2 - 1,)),
            pltpu.SemaphoreType.DMA((halves * (links + slabs // 2 - 1),)),
            pltpu.SemaphoreType.DMA((3,)),
            pltpu.SemaphoreType.REGULAR,
        ],
        compiler_params=pltpu.CompilerParams(collective_id=0, has_side_effects=True),
        name="sweeps",
    )(right_side, inverse_factor, forward_trace, backward_trace, margin)
    return pl.pallas_call(
        finish,
        out_shape=jax.ShapeDtypeStruct(right_side.shape, F32),
        in_specs=[pl.BlockSpec(memory_space=pltpu.VMEM)] * 2,
        out_specs=hbm,
        scratch_shapes=[pltpu.VMEM((m // KMAX, cols, KMAX), F32), pltpu.SemaphoreType.DMA((m // KMAX,))],
        compiler_params=pltpu.CompilerParams(vmem_limit_bytes=16 << 20),
        name="finish",
    )(half, inverse_factor)


def solution(mesh):
    four = P("slab", "patch", None, None)
    return jax.shard_map(
        functools.partial(on_device, mesh.shape["slab"], mesh.shape["patch"]),
        mesh=mesh,
        in_specs=(four, four, four, four, P("slab", "patch")),
        out_specs=four,
        check_vma=False,
    )
```

```python
import functools

import jax
import jax.numpy as jnp
from jax import lax
from jax.experimental import pallas as pl
from jax.experimental.pallas import tpu as pltpu
from jax.sharding import PartitionSpec as P

KMAX = 256
BF = jnp.bfloat16
F32 = jnp.float32
MESH = pl.DeviceIdType.MESH


def nt(a, b):
    return lax.dot_general(a, b, (((1,), (1,)), ((), ())), preferred_element_type=F32)


def nn(a, b):
    return lax.dot_general(a, b, (((1,), (0,)), ((), ())), preferred_element_type=F32)


def tn(a, b):
    return lax.dot_general(a, b, (((0,), (0,)), ((), ())), preferred_element_type=F32)


def halfway(x, fac, m):
    return jnp.concatenate(
        [nt(x[:, : i + KMAX], fac[i : i + KMAX, : i + KMAX]).astype(BF) for i in range(0, m, KMAX)],
        axis=1,
    )


def solve(x, fac, m):
    half = halfway(x, fac, m)
    return [nn(half[:, k:], fac[k:, k : k + KMAX]) for k in range(0, m, KMAX)]


def finish(half_ref, l_ref, out_ref, held, sem):
    m = half_ref.shape[1]
    copies = []
    for n, k in enumerate(range(0, m, KMAX)):
        held[n] = nn(half_ref[:, k:], l_ref[0, 0, k:, k : k + KMAX])
        copies.append(pltpu.make_async_copy(held.at[n], out_ref.at[0, 0, :, k : k + KMAX], sem.at[n]))
        copies[-1].start()
    for c in copies:
        c.wait()


FAR_LEFT, FAR_RIGHT, LEFT, RIGHT, OWN = range(5)
HOST, AIDE = 1, 2


class Names:
    def __init__(self):
        self.count = 0

    def take(self):
        self.count += 1
        return self.count - 1


def kernel(
    slabs, patches, halves,
    r_hbm, l_hbm, f_hbm, b_hbm, margin_ref, out_ref,
    r_v, fac, maps,
    tail_s, head_s, zt_s, zh_s, d_s,
    side_r, z_r, d_home, u_home,
    a_h, b_h, t_h, v_h, w_h, d_h, u_h, u0_s,
    adj, gt, place, zr, lent, effect,
    load_sem, send_sem, near_sem, home_sem, op_sem, term_sem, ring_sem, aide_sem, turn_sem,
):
    s = lax.axis_index("slab")
    q = lax.axis_index("patch")
    left = lax.rem(q + patches - 1, patches)
    right = lax.rem(q + 1, patches)
    next_left = lax.rem(q + patches - 2, patches)
    next_right = lax.rem(q + 2, patches)
    pair = s + 1 - 2 * lax.rem(s, 2)
    odd = lax.rem(s, 2) == 1
    m = fac.shape[-1]
    face = f_hbm.shape[-2]
    cols = r_v.shape[0]
    top = slabs - 1
    wide = cols // halves
    inner_low, inner_high = s > 0, s < top
    first_slab = s == 0
    host, guest, last = s == HOST, s > HOST, s == top
    odd_guest = guest & odd
    aide = s == AIDE

    steps = range(0, m, KMAX)
    r_load = pltpu.make_async_copy(r_hbm.at[0, 0], r_v, load_sem.at[0])
    l_loads = []
    for n, i in enumerate(steps):
        block = (pl.ds(i, KMAX), pl.ds(0, i + KMAX))
        l_loads.append(pltpu.make_async_copy(l_hbm.at[(0, 0, *block)], fac.at[block], load_sem.at[1 + n]))
    map_loads = [
        pltpu.make_async_copy(f_hbm.at[0, 0], maps.at[:face], load_sem.at[0]),
        pltpu.make_async_copy(b_hbm.at[0, 0], maps.at[face:], load_sem.at[0]),
    ]
    barrier = pltpu.get_barrier_semaphore()

    def greet(slab, patch):
        pl.semaphore_signal(barrier, inc=1, device_id=(slab, patch), device_id_type=MESH)

    greet(s, left)
    greet(s, right)
    greet(pair, q)

    @pl.when(first_slab)
    def _():
        greet(HOST, left)
        greet(HOST, right)
        greet(AIDE, q)

    @pl.when(aide)
    def _():
        greet(0, q)

    @pl.when(guest)
    def _():
        greet(HOST, q)

    @pl.when(odd_guest)
    def _():
        greet(HOST, left)
        greet(HOST, right)

    @pl.when(host)
    def _():
        greet(s, next_left)
        greet(s, next_right)
        greet(0, left)
        greet(0, right)
        for t in range(HOST + 1, slabs):
            greet(t, q)
        for t in range(HOST + 2, slabs, 2):
            greet(t, left)
            greet(t, right)

    r_load.start()
    for c in l_loads:
        c.start()

    greeted = (
        3
        + first_slab.astype(jnp.int32) * 3
        + aide.astype(jnp.int32)
        + guest.astype(jnp.int32)
        + odd_guest.astype(jnp.int32) * 2
        + host.astype(jnp.int32) * (4 + slabs - 2 + 2 * len(range(HOST + 2, slabs, 2)))
    )

    names = Names()

    class Group:
        def __init__(self, whole, copies):
            self.whole, self.sem = whole, send_sem.at[names.take()]
            self.copies = [
                pltpu.make_async_remote_copy(
                    src_ref=src, dst_ref=dst, send_sem=self.sem, recv_sem=recv, device_id=place, device_id_type=MESH
                )
                for src, dst, recv, place in copies
            ]

        def start(self, first=0, end=None):
            for c in self.copies[first:end]:
                c.start()

        def sent(self):
            arrived(self.whole, self.sem)

    def arrived(ref, sem):
        pltpu.make_async_copy(ref, ref, sem).wait()

    def start(*groups):
        for c in groups:
            c.start()

    def sent(*groups):
        for c in groups:
            c.sent()

    part = [pl.ds(g * wide, wide) for g in range(halves)]
    both = range(halves)
    low_rows, high_rows = pl.ds(0, face), pl.ds(face, face)
    two, four, middle = pl.ds(0, 2), pl.ds(0, 4), pl.ds(2, 3)

    tail_c = [
        Group(
            tail_s,
            [
                (tail_s.at[w], side_r.at[0, w], near_sem.at[g], (s, right)),
                (head_s.at[w], side_r.at[1, w], near_sem.at[g], (s, left)),
            ],
        )
        for g, w in enumerate(part)
    ]

    def z_rows(rows, n):
        return Group(
            zt_s,
            [
                (zt_s.at[rows], z_r.at[0, rows], near_sem.at[halves + n], (s, right)),
                (zh_s.at[rows], z_r.at[1, rows], near_sem.at[halves + n], (s, left)),
            ],
        )

    zd_c, zu_c = z_rows(low_rows, 0), z_rows(high_rows, 1)
    shared = names.count

    seed_c = Group(
        d_h.at[0, :, middle],
        [
            (d_s.at[w], d_h.at[0, g, j], ring_sem.at[g], (HOST, p))
            for g, w in enumerate(part)
            for j, p in ((LEFT, right), (RIGHT, left), (OWN, q))
        ],
    )
    lent_c = Group(
        zt_s,
        [
            (zt_s.at[high_rows], lent.at[0], aide_sem.at[0], (AIDE, q)),
            (zh_s.at[high_rows], lent.at[1], aide_sem.at[0], (AIDE, q)),
        ],
    )
    most = names.count

    names.count = shared
    below = jnp.maximum(s - 1, 0)
    inner = jnp.maximum(s - 2, 0)
    inners = slabs - 3
    sides = ((0, right), (1, left))
    t_sem, v_sem, w_sem = 0, inners, 2 * inners
    a_sem, b_sem, k_sem = 0, halves * inners, halves * inners + slabs - 2
    t_c = Group(t_h.at[below], [(t_h.at[below], t_h.at[below], op_sem.at[t_sem + inner], (HOST, q))])
    v_c = Group(v_h.at[below], [(v_h.at[below], v_h.at[below], op_sem.at[v_sem + inner], (HOST, q))])
    w_to = op_sem.at[w_sem + below]
    w_c = Group(w_h.at[below, 2], [(w_h.at[below, 2], w_h.at[below, 2], w_to, (HOST, q))])
    w_near = Group(w_h.at[below, two], [(w_h.at[below, 2], w_h.at[below, j], w_to, (HOST, p)) for j, p in sides])
    a_c = Group(
        a_h.at[below],
        [(a_h.at[below, g], a_h.at[below, g], term_sem.at[a_sem + halves * inner + g], (HOST, q)) for g in both],
    )
    b_to = term_sem.at[b_sem + inner]
    b_c = Group(b_h.at[below, :, 2], [(b_h.at[below, g, 2], b_h.at[below, g, 2], b_to, (HOST, q)) for g in both])
    b_swap = Group(
        b_h.at[below, :, two],
        [(b_h.at[below, g, 2], b_h.at[below, g, j], near_sem.at[halves + 2], (s, p)) for g in both for j, p in sides],
    )
    b_pass = Group(
        b_h.at[below, :, two],
        [(b_h.at[below, :, two], b_h.at[below, :, two], b_to, (HOST, q))],
    )
    lent_near = Group(
        lent.at[two],
        [
            (lent.at[0], lent.at[2], aide_sem.at[1], (AIDE, right)),
            (lent.at[1], lent.at[3], aide_sem.at[2], (AIDE, left)),
        ],
    )
    lent_back = Group(
        lent.at[two],
        [(lent.at[2 + n], z_r.at[n, high_rows], near_sem.at[halves + 1], (0, q)) for n in range(2)],
    )
    most = max(most, names.count)

    names.count = shared
    close = ((LEFT, right), (RIGHT, left))
    far = close + ((FAR_LEFT, next_right), (FAR_RIGHT, next_left))
    up_rings = range(1, top - 1, 2)

    def ring_of(kind, t):
        return halves * (t - 1) if kind == 0 else halves * (slabs - 1 + up_rings.index(t))

    def around(buf, t, kind, places):
        return Group(
            buf.at[t - 1, :, pl.ds(0, len(places))],
            [
                (buf.at[t - 1, g, OWN], buf.at[t - 1, g, j], ring_sem.at[ring_of(kind, t) + g], (s, p))
                for g in both
                for j, p in places
            ],
        )

    round_d = {t: around(d_h, t, 0, far if t == top else close) for t in range(2, slabs)}
    round_u = {t: around(u_h, t, 1, far) for t in up_rings}
    kept_c = {
        t: Group(
            b_h.at[t - 1, :, two],
            [
                (b_h.at[t - 1, g, 2], b_h.at[t - 1, g, j], term_sem.at[k_sem + t // 2], (s, p))
                for g in both
                for j, p in sides
            ],
        )
        for t in range(1, top, 2)
    }
    w_host = Group(w_h.at[0, two], [(w_h.at[0, 2], w_h.at[0, j], op_sem.at[w_sem], (s, p)) for j, p in sides])

    def back(buf, dst, recv, t):
        return Group(
            buf.at[t - 1, :, middle], [(buf.at[t - 1, g, middle], dst.at[g], recv, (t, q)) for g in both]
        )

    back_d = {t: back(d_h, d_home, home_sem.at[0], t) for t in range(2, slabs)}
    back_u = {t: back(u_h, u_home, home_sem.at[1], t) for t in range(2, top)}
    last_u = Group(u0_s, [(u0_s.at[g], u_home.at[g], home_sem.at[1 + g], (0, q)) for g in both])
    most = max(most, names.count)
    assert most == send_sem.shape[0], most

    count = margin_ref[0, 0]
    row = lax.broadcasted_iota(jnp.int32, (KMAX, KMAX), 0)
    col = lax.broadcasted_iota(jnp.int32, (KMAX, KMAX), 1)
    hit = (row == KMAX - count + col) & (col < count)
    place[...] = jnp.where(hit, 1.0, 0.0).astype(BF)

    r_load.wait()
    for c in l_loads:
        c.wait()
    for c in map_loads:
        c.start()
    half = halfway(r_v[...].astype(BF), fac, m)
    at_tail = nn(half[:, m - KMAX :], fac[m - KMAX :, m - KMAX :]).astype(BF)
    tail_s[...] = nn(at_tail, place[...]).astype(BF)
    head_s[...] = nn(half, fac[:, :KMAX]).astype(BF)

    pl.semaphore_wait(barrier, greeted)

    def send_tails():
        start(*tail_c)

    pl.when(first_slab)(send_tails)

    low = fac[:, :face]
    high = fac[m - face :, m - face :]
    k_tail = jnp.concatenate(
        [tn(low[m - KMAX :], fac[m - KMAX :, m - KMAX :]), tn(high, fac[m - face :, m - KMAX :])], axis=0
    )
    k_head = jnp.concatenate([tn(low, fac[:, :KMAX]), tn(high, fac[m - face :, :KMAX])], axis=0)
    zt_s[...] = nn(k_tail.astype(BF), place[...]).astype(BF)
    zh_s[...] = k_head.astype(BF)

    far_right, far_left = q == patches - 1, q == 0

    def lift_far():
        @pl.when(far_right)
        def _():
            zu_c.start(0, 1)

        @pl.when(far_left)
        def _():
            zu_c.start(1, 2)

    def lift():
        @pl.when(~far_right)
        def _():
            zu_c.start(0, 1)

        @pl.when(~far_left)
        def _():
            zu_c.start(1, 2)

    @pl.when(inner_low)
    def _():
        start(zd_c)

    pl.when(guest & inner_high)(lift_far)

    arrived(maps, load_sem.at[0])
    for k, piece in enumerate(solve(maps[...], fac, m)):
        gt[:, k * KMAX : (k + 1) * KMAX] = piece.astype(BF)

    @pl.when(guest)
    def _():
        zd_c.sent()
        send_tails()

    @pl.when(first_slab)
    def _():
        tail_c[0].sent()
        pl.semaphore_signal(turn_sem, inc=1, device_id=(HOST, q), device_id_type=MESH)

    @pl.when(host)
    def _():
        pl.semaphore_wait(turn_sem, 1)
        send_tails()

    @pl.when(inner_low)
    def _():
        arrived(z_r.at[:, low_rows], near_sem.at[halves])
        zr[low_rows] = nt(z_r[1, low_rows], place[...]).astype(BF)
        own = (-gt[:, :face].astype(F32)).T.astype(BF)
        from_left = (0.5 * nt(z_r[0, low_rows], gt[:, :KMAX])).astype(BF)
        from_right = (0.5 * nt(zr[low_rows], gt[:, m - KMAX :])).astype(BF)
        for n, block in enumerate((own, from_left, from_right)):
            lines = pl.ds(n * face, face)
            t_h[below, lines] = block[:, :face]

            @pl.when(inner_high)
            def _():
                v_h[below, lines] = block[:, face:]

            @pl.when(~inner_high)
            def _():
                w_h[below, 2, lines] = block[:, face:]

        @pl.when(guest & inner_high)
        def _():
            start(t_c, v_c)

        @pl.when(last)
        def _():
            start(w_c)

    for g, w in enumerate(part):
        arrived(side_r.at[:, w], near_sem.at[g])
        adj[w, :] = r_v[w, :]
        adj[w, :KMAX] = adj[w, :KMAX] - 0.5 * side_r[0, w].astype(F32)
        adj[w, m - KMAX :] = adj[w, m - KMAX :] - 0.5 * nt(side_r[1, w], place[...])

        @pl.when(first_slab)
        def _():
            d_s[w] = nt(adj[w, :].astype(BF), gt[:face]).astype(BF)
            seed_c.start(3 * g, 3 * g + 3)

        @pl.when(inner_low)
        def _():
            terms = nt(adj[w, :].astype(BF), gt[...]).astype(BF)
            a_h[below, g] = terms[:, :face]
            b_h[below, g, 2] = terms[:, face:]

            @pl.when(guest & inner_high)
            def _():
                a_c.start(g, g + 1)
                if g == 0:
                    lift()

            @pl.when(guest)
            def _():
                b_c.start(g, g + 1)

            @pl.when(last)
            def _():
                b_swap.start(2 * g, 2 * g + 2)

    @pl.when(last)
    def _():
        start(w_near)
        arrived(b_h.at[below, :, two], near_sem.at[halves + 2])
        start(b_pass)

    @pl.when(first_slab)
    def _():
        start(lent_c)
        for k, piece in enumerate(solve(adj[...].astype(BF), fac, m)):
            out_ref[0, 0, :, k * KMAX : (k + 1) * KMAX] = piece
        effect[:face] = (-tn(fac[m - face :, m - face :], fac[m - face :, :])).astype(BF)

    def make_up():
        arrived(z_r.at[:, high_rows], near_sem.at[halves + 1])
        zr[high_rows] = nt(z_r[1, high_rows], place[...]).astype(BF)

        @pl.when(inner_low)
        def _():
            w_h[below, 2, :face] = (-gt[face:, m - face :].astype(F32)).T.astype(BF)
            w_h[below, 2, face : 2 * face] = (0.5 * nt(z_r[0, high_rows], gt[face:, :KMAX])).astype(BF)
            w_h[below, 2, 2 * face :] = (0.5 * nt(zr[high_rows], gt[face:, m - KMAX :])).astype(BF)

    @pl.when(guest & inner_high)
    def _():
        make_up()
        start(w_c)

        @pl.when(odd)
        def _():
            start(w_near)

    @pl.when(aide)
    def _():
        arrived(lent.at[two], aide_sem.at[0])
        start(lent_near)

        @pl.when(q == 0)
        def _():
            arrived(lent.at[3], aide_sem.at[2])
            lent_back.start(1, 2)
            arrived(lent.at[2], aide_sem.at[1])
            lent_back.start(0, 1)

        @pl.when(q > 0)
        def _():
            arrived(lent.at[2], aide_sem.at[1])
            lent_back.start(0, 1)
            arrived(lent.at[3], aide_sem.at[2])
            lent_back.start(1, 2)

    def beside(ref, n, g, slots):
        return jnp.concatenate([ref[n, g, j] for j in slots], axis=1)

    centre = (OWN, LEFT, RIGHT)

    def drop_low(get):
        for g, w in enumerate(part):
            adj[w, :face] = adj[w, :face] - get(g, 2).astype(F32)
            adj[w, :KMAX] = adj[w, :KMAX] + 0.5 * nn(get(g, 0), z_r[0, low_rows])
            adj[w, m - KMAX :] = adj[w, m - KMAX :] + 0.5 * nn(get(g, 1), zr[low_rows])

    def drop_high(g, get):
        w = part[g]
        adj[w, m - face :] = adj[w, m - face :] - get(g, 2).astype(F32)
        adj[w, :KMAX] = adj[w, :KMAX] + 0.5 * nn(get(g, 0), z_r[0, high_rows])
        adj[w, m - KMAX :] = adj[w, m - KMAX :] + 0.5 * nn(get(g, 1), zr[high_rows])

    @pl.when(host)
    def _():
        for t in range(1, top):
            n = t - 1
            if t > HOST:
                arrived(t_h.at[n], op_sem.at[t_sem + n - 1])
            for g in both:
                if t > HOST:
                    arrived(a_h.at[n, g], term_sem.at[a_sem + halves * (n - 1) + g])
                arrived(d_h.at[n, g, pl.ds(2, 3 if t == 1 else 2)], ring_sem.at[ring_of(0, t) + g])
                d_h[n + 1, g, OWN] = (a_h[n, g].astype(F32) + nn(beside(d_h, n, g, centre), t_h[n])).astype(BF)
                per = len(far if t + 1 == top else close)
                round_d[t + 1].start(per * g, per * g + per)
            if t == 1:
                start(zu_c)
            if t > HOST:
                back_d[t].start()
                if t % 2 == 0:
                    kept_c[t - 1].start()
                arrived(v_h.at[n], op_sem.at[v_sem + n - 1])
                arrived(b_h.at[n, :, 2], term_sem.at[b_sem + n - 1])
            for g in both:
                b_h[n, g, 2] = (b_h[n, g, 2].astype(F32) + nn(beside(d_h, n, g, centre), v_h[n])).astype(BF)
            if t == min(2, top - 1):
                make_up()
                start(w_host)

        drop_low(lambda g, j: d_h[0, g, 2 + j])
        arrived(w_h.at[top - 1], op_sem.at[w_sem + top - 1])
        for t in range(top, 0, -2):
            n = t - 1
            state = d_h if t == top else u_h
            if t < top:
                arrived(w_h.at[n, two] if t == HOST else w_h.at[n], op_sem.at[w_sem + n])
            if t > 1:
                arrived(w_h.at[n - 1, 2], op_sem.at[w_sem + n - 1])
            if t == top:
                arrived(b_h.at[n], term_sem.at[b_sem + n - 1])
            else:
                arrived(b_h.at[n, :, two], term_sem.at[k_sem + t // 2])
            for g in both:
                arrived(state.at[n, g, four], ring_sem.at[ring_of(0 if t == top else 1, t) + g])
                for j, slots in enumerate(((LEFT, FAR_LEFT, OWN), (RIGHT, OWN, FAR_RIGHT), centre)):
                    u = (b_h[n, g, j].astype(F32) + nn(beside(state, n, g, slots), w_h[n, j])).astype(BF)
                    if t > 1:
                        u_h[n - 1, g, 2 + j] = u
                    else:
                        u0_s[g, j] = u
                if t > 1:
                    u = b_h[n - 1, g, 2].astype(F32) + nn(beside(u_h, n - 1, g, centre), w_h[n - 1, 2])
                    u_h[n - 2, g, OWN] = u.astype(BF)
                    round_u[t - 2].start(4 * g, 4 * g + 4)
                    back_u[t - 1].start(g, g + 1)
                else:
                    last_u.start(g, g + 1)
                if t > HOST:
                    (back_d if t == top else back_u)[t].start(g, g + 1)

    @pl.when(host)
    def _():
        if HOST < top:
            for g in both:
                drop_high(g, lambda g, j: u_h[0, g, 2 + j])

    @pl.when(guest)
    def _():
        arrived(d_home, home_sem.at[0])
        drop_low(lambda g, j: d_home[g, j])

    @pl.when(guest & inner_high)
    def _():
        arrived(u_home, home_sem.at[1])
        for g in both:
            drop_high(g, lambda g, j: u_home[g, j])

    @pl.when(first_slab)
    def _():
        arrived(z_r.at[:, high_rows], near_sem.at[halves + 1])
        half = jnp.concatenate(
            [nt(z_r[0, high_rows], fac[i : i + KMAX, :KMAX]).astype(BF) for i in range(0, m, KMAX)], axis=1
        )
        for k in range(0, m, KMAX):
            spread = 0.5 * nn(half[:, k:], fac[k:, k : k + KMAX])
            effect[face : 2 * face, k : k + KMAX] = spread.astype(BF)
        at_tail = nt(z_r[1, high_rows], place[...]).astype(BF)
        half = nt(at_tail, fac[m - KMAX :, m - KMAX :]).astype(BF)
        effect[2 * face :] = (0.5 * nn(half, fac[m - KMAX :, :])).astype(BF)
        for g, w in enumerate(part):
            arrived(u_home.at[g], home_sem.at[1 + g])
            u = jnp.concatenate([u_home[g, j] for j in (2, 0, 1)], axis=1)
            out_ref[0, 0, w, :] = out_ref[0, 0, w, :] + nn(u, effect[...])

    @pl.when(inner_low)
    def _():
        for k, piece in enumerate(solve(adj[...].astype(BF), fac, m)):
            out_ref[0, 0, :, k * KMAX : (k + 1) * KMAX] = piece

    @pl.when(first_slab)
    def _():
        sent(tail_c[1], lent_c, seed_c)

    @pl.when(inner_low)
    def _():
        sent(tail_c[1])

    @pl.when(host)
    def _():
        sent(zd_c, tail_c[0])

    @pl.when(guest)
    def _():
        sent(tail_c[0])

    @pl.when(inner_low & inner_high)
    def _():
        sent(zu_c)

    @pl.when(aide)
    def _():
        sent(lent_near, lent_back)

    @pl.when(guest)
    def _():
        sent(w_c, b_c)

    @pl.when(guest & inner_high)
    def _():
        sent(t_c, v_c, a_c)

    @pl.when(odd_guest)
    def _():
        sent(w_near)

    @pl.when(last)
    def _():
        sent(b_swap, b_pass)

    @pl.when(host)
    def _():
        sent(w_host, last_u)
        for kind in (round_d, round_u, kept_c, back_d, back_u):
            sent(*kind.values())


def on_device(slabs, patches, right_side, inverse_factor, forward_trace, backward_trace, margin):
    cols, m = right_side.shape[2:]
    face = forward_trace.shape[2]
    halves = 2
    rows = cols // halves
    links = slabs - 1
    wide = pltpu.VMEM((cols, KMAX), BF)
    square = pltpu.VMEM((2 * face, KMAX), BF)
    hbm = pl.BlockSpec(memory_space=pltpu.HBM)
    home = pltpu.VMEM((halves, 3, rows, face), BF)
    ops = pltpu.VMEM((links, 3 * face, face), BF)
    ring = pltpu.VMEM((links, halves, 5, rows, face), BF)
    sends = halves + 2 + max(10, 2 * (links - 1) + (links - 2) + 3 * (slabs // 2 - 1) - (slabs // 2 - 1) + 2)
    return pl.pallas_call(
        functools.partial(kernel, slabs, patches, halves),
        out_shape=pltpu.VMEM(right_side.shape, F32),
        in_specs=[hbm, hbm, hbm, hbm, pl.BlockSpec(memory_space=pltpu.SMEM)],
        out_specs=pl.BlockSpec(memory_space=pltpu.VMEM),
        scratch_shapes=[
            pltpu.VMEM((cols, m), F32),
            pltpu.VMEM((m, m), BF),
            pltpu.VMEM((2 * face, m), BF),
            wide, wide, square, square, pltpu.VMEM((cols, face), BF),
            pltpu.VMEM((2, cols, KMAX), BF), pltpu.VMEM((2, 2 * face, KMAX), BF), home, home,
            pltpu.VMEM((links, halves, rows, face), BF),
            pltpu.VMEM((links, halves, 3, rows, face), BF),
            ops, ops, pltpu.VMEM((links, 3, 3 * face, face), BF),
            ring, ring, home,
            pltpu.VMEM((cols, m), F32),
            pltpu.VMEM((2 * face, m), BF),
            pltpu.VMEM((KMAX, KMAX), BF),
            square,
            pltpu.VMEM((4, face, KMAX), BF),
            pltpu.VMEM((3 * face, m), BF),
            pltpu.SemaphoreType.DMA((2 + m // KMAX,)),
            pltpu.SemaphoreType.DMA((sends,)),
            pltpu.SemaphoreType.DMA((halves + 3,)),
            pltpu.SemaphoreType.DMA((1 + halves,)),
            pltpu.SemaphoreType.DMA((2 * (links - 2) + links,)),
            pltpu.SemaphoreType.DMA((halves * (links - 2) + links - 1 + slabs // 2 - 1,)),
            pltpu.SemaphoreType.DMA((halves * (links + slabs // 2 - 1),)),
            pltpu.SemaphoreType.DMA((3,)),
            pltpu.SemaphoreType.REGULAR,
        ],
        compiler_params=pltpu.CompilerParams(collective_id=0, has_side_effects=True),
        name="sweeps",
    )(right_side, inverse_factor, forward_trace, backward_trace, margin)
    return pl.pallas_call(
        finish,
        out_shape=jax.ShapeDtypeStruct(right_side.shape, F32),
        in_specs=[pl.BlockSpec(memory_space=pltpu.VMEM)] * 2,
        out_specs=hbm,
        scratch_shapes=[pltpu.VMEM((m // KMAX, cols, KMAX), F32), pltpu.SemaphoreType.DMA((m // KMAX,))],
        compiler_params=pltpu.CompilerParams(vmem_limit_bytes=16 << 20),
        name="finish",
    )(half, inverse_factor)


def solution(mesh):
    four = P("slab", "patch", None, None)
    return jax.shard_map(
        functools.partial(on_device, mesh.shape["slab"], mesh.shape["patch"]),
        mesh=mesh,
        in_specs=(four, four, four, four, P("slab", "patch")),
        out_specs=four,
        check_vma=False,
    )
```

```python
import functools

import jax
import jax.numpy as jnp
from jax import lax
from jax.experimental import pallas as pl
from jax.experimental.pallas import tpu as pltpu
from jax.sharding import PartitionSpec as P

KMAX = 256
BF = jnp.bfloat16
F32 = jnp.float32
MESH = pl.DeviceIdType.MESH


def nt(a, b):
    return lax.dot_general(a, b, (((1,), (1,)), ((), ())), preferred_element_type=F32)


def nn(a, b):
    return lax.dot_general(a, b, (((1,), (0,)), ((), ())), preferred_element_type=F32)


def tn(a, b):
    return lax.dot_general(a, b, (((0,), (0,)), ((), ())), preferred_element_type=F32)


def halfway(x, fac, m):
    return jnp.concatenate(
        [nt(x[:, : i + KMAX], fac[i : i + KMAX, : i + KMAX]).astype(BF) for i in range(0, m, KMAX)],
        axis=1,
    )


def solve(x, fac, m):
    half = halfway(x, fac, m)
    return [nn(half[:, k:], fac[k:, k : k + KMAX]) for k in range(0, m, KMAX)]


def finish(half_ref, l_ref, out_ref, held, sem):
    m = half_ref.shape[1]
    copies = []
    for n, k in enumerate(range(0, m, KMAX)):
        held[n] = nn(half_ref[:, k:], l_ref[0, 0, k:, k : k + KMAX])
        copies.append(pltpu.make_async_copy(held.at[n], out_ref.at[0, 0, :, k : k + KMAX], sem.at[n]))
        copies[-1].start()
    for c in copies:
        c.wait()


FAR_LEFT, FAR_RIGHT, LEFT, RIGHT, OWN = range(5)
HOST, AIDE = 1, 2


class Names:
    def __init__(self):
        self.count = 0

    def take(self):
        self.count += 1
        return self.count - 1


def kernel(
    slabs, patches, halves,
    r_hbm, l_hbm, f_hbm, b_hbm, margin_ref, out_ref,
    r_v, fac, maps,
    tail_s, head_s, zt_s, zh_s, d_s,
    side_r, z_r, d_home, u_home,
    a_h, b_h, t_h, v_h, w_h, d_h, u_h, u0_s,
    adj, gt, place, zr, lent, effect,
    load_sem, send_sem, near_sem, home_sem, op_sem, term_sem, ring_sem, aide_sem, turn_sem,
):
    s = lax.axis_index("slab")
    q = lax.axis_index("patch")
    left = lax.rem(q + patches - 1, patches)
    right = lax.rem(q + 1, patches)
    next_left = lax.rem(q + patches - 2, patches)
    next_right = lax.rem(q + 2, patches)
    pair = s + 1 - 2 * lax.rem(s, 2)
    odd = lax.rem(s, 2) == 1
    m = fac.shape[-1]
    face = f_hbm.shape[-2]
    cols = r_v.shape[0]
    top = slabs - 1
    wide = cols // halves
    inner_low, inner_high = s > 0, s < top
    first_slab = s == 0
    host, guest, last = s == HOST, s > HOST, s == top
    odd_guest = guest & odd
    aide = s == AIDE

    steps = range(0, m, KMAX)
    r_load = pltpu.make_async_copy(r_hbm.at[0, 0], r_v, load_sem.at[0])
    l_loads = []
    for n, i in enumerate(steps):
        block = (pl.ds(i, KMAX), pl.ds(0, i + KMAX))
        l_loads.append(pltpu.make_async_copy(l_hbm.at[(0, 0, *block)], fac.at[block], load_sem.at[1 + n]))
    map_loads = [
        pltpu.make_async_copy(f_hbm.at[0, 0], maps.at[:face], load_sem.at[0]),
        pltpu.make_async_copy(b_hbm.at[0, 0], maps.at[face:], load_sem.at[0]),
    ]
    barrier = pltpu.get_barrier_semaphore()

    def greet(slab, patch):
        pl.semaphore_signal(barrier, inc=1, device_id=(slab, patch), device_id_type=MESH)

    greet(s, left)
    greet(s, right)
    greet(pair, q)

    @pl.when(first_slab)
    def _():
        greet(HOST, left)
        greet(HOST, right)
        greet(AIDE, q)

    @pl.when(aide)
    def _():
        greet(0, q)

    @pl.when(guest)
    def _():
        greet(HOST, q)

    @pl.when(odd_guest)
    def _():
        greet(HOST, left)
        greet(HOST, right)

    @pl.when(host)
    def _():
        greet(s, next_left)
        greet(s, next_right)
        greet(0, left)
        greet(0, right)
        for t in range(HOST + 1, slabs):
            greet(t, q)
        for t in range(HOST + 2, slabs, 2):
            greet(t, left)
            greet(t, right)

    r_load.start()
    for c in l_loads:
        c.start()

    greeted = (
        3
        + first_slab.astype(jnp.int32) * 3
        + aide.astype(jnp.int32)
        + guest.astype(jnp.int32)
        + odd_guest.astype(jnp.int32) * 2
        + host.astype(jnp.int32) * (4 + slabs - 2 + 2 * len(range(HOST + 2, slabs, 2)))
    )

    names = Names()

    class Group:
        def __init__(self, whole, copies):
            self.whole, self.sem = whole, send_sem.at[names.take()]
            self.copies = [
                pltpu.make_async_remote_copy(
                    src_ref=src, dst_ref=dst, send_sem=self.sem, recv_sem=recv, device_id=place, device_id_type=MESH
                )
                for src, dst, recv, place in copies
            ]

        def start(self, first=0, end=None):
            for c in self.copies[first:end]:
                c.start()

        def sent(self):
            arrived(self.whole, self.sem)

    def arrived(ref, sem):
        pltpu.make_async_copy(ref, ref, sem).wait()

    def start(*groups):
        for c in groups:
            c.start()

    def sent(*groups):
        for c in groups:
            c.sent()

    part = [pl.ds(g * wide, wide) for g in range(halves)]
    both = range(halves)
    low_rows, high_rows = pl.ds(0, face), pl.ds(face, face)
    two, four, middle = pl.ds(0, 2), pl.ds(0, 4), pl.ds(2, 3)

    tail_c = [
        Group(
            tail_s,
            [
                (tail_s.at[w], side_r.at[0, w], near_sem.at[g], (s, right)),
                (head_s.at[w], side_r.at[1, w], near_sem.at[g], (s, left)),
            ],
        )
        for g, w in enumerate(part)
    ]

    def z_rows(rows, n):
        return Group(
            zt_s,
            [
                (zt_s.at[rows], z_r.at[0, rows], near_sem.at[halves + n], (s, right)),
                (zh_s.at[rows], z_r.at[1, rows], near_sem.at[halves + n], (s, left)),
            ],
        )

    zd_c, zu_c = z_rows(low_rows, 0), z_rows(high_rows, 1)
    shared = names.count

    seed_c = Group(
        d_h.at[0, :, middle],
        [
            (d_s.at[w], d_h.at[0, g, j], ring_sem.at[g], (HOST, p))
            for g, w in enumerate(part)
            for j, p in ((LEFT, right), (RIGHT, left), (OWN, q))
        ],
    )
    lent_c = Group(
        zt_s,
        [
            (zt_s.at[high_rows], lent.at[0], aide_sem.at[0], (AIDE, q)),
            (zh_s.at[high_rows], lent.at[1], aide_sem.at[0], (AIDE, q)),
        ],
    )
    most = names.count

    names.count = shared
    below = jnp.maximum(s - 1, 0)
    inner = jnp.maximum(s - 2, 0)
    inners = slabs - 3
    sides = ((0, right), (1, left))
    t_sem, v_sem, w_sem = 0, inners, 2 * inners
    a_sem, b_sem, k_sem = 0, halves * inners, halves * inners + slabs - 2
    t_c = Group(t_h.at[below], [(t_h.at[below], t_h.at[below], op_sem.at[t_sem + inner], (HOST, q))])
    v_c = Group(v_h.at[below], [(v_h.at[below], v_h.at[below], op_sem.at[v_sem + inner], (HOST, q))])
    w_to = op_sem.at[w_sem + below]
    w_c = Group(w_h.at[below, 2], [(w_h.at[below, 2], w_h.at[below, 2], w_to, (HOST, q))])
    w_near = Group(w_h.at[below, two], [(w_h.at[below, 2], w_h.at[below, j], w_to, (HOST, p)) for j, p in sides])
    a_c = Group(
        a_h.at[below],
        [(a_h.at[below, g], a_h.at[below, g], term_sem.at[a_sem + halves * inner + g], (HOST, q)) for g in both],
    )
    b_to = term_sem.at[b_sem + inner]
    b_c = Group(b_h.at[below, :, 2], [(b_h.at[below, g, 2], b_h.at[below, g, 2], b_to, (HOST, q)) for g in both])
    b_swap = Group(
        b_h.at[below, :, two],
        [(b_h.at[below, g, 2], b_h.at[below, g, j], near_sem.at[halves + 2], (s, p)) for g in both for j, p in sides],
    )
    b_pass = Group(
        b_h.at[below, :, two],
        [(b_h.at[below, :, two], b_h.at[below, :, two], b_to, (HOST, q))],
    )
    lent_near = Group(
        lent.at[two],
        [
            (lent.at[0], lent.at[2], aide_sem.at[1], (AIDE, right)),
            (lent.at[1], lent.at[3], aide_sem.at[2], (AIDE, left)),
        ],
    )
    lent_back = Group(
        lent.at[two],
        [(lent.at[2 + n], z_r.at[n, high_rows], near_sem.at[halves + 1], (0, q)) for n in range(2)],
    )
    most = max(most, names.count)

    names.count = shared
    close = ((LEFT, right), (RIGHT, left))
    far = close + ((FAR_LEFT, next_right), (FAR_RIGHT, next_left))
    up_rings = range(1, top - 1, 2)

    def ring_of(kind, t):
        return halves * (t - 1) if kind == 0 else halves * (slabs - 1 + up_rings.index(t))

    def around(buf, t, kind, places):
        return Group(
            buf.at[t - 1, :, pl.ds(0, len(places))],
            [
                (buf.at[t - 1, g, OWN], buf.at[t - 1, g, j], ring_sem.at[ring_of(kind, t) + g], (s, p))
                for g in both
                for j, p in places
            ],
        )

    round_d = {t: around(d_h, t, 0, far if t == top else close) for t in range(2, slabs)}
    round_u = {t: around(u_h, t, 1, far) for t in up_rings}
    kept_c = {
        t: Group(
            b_h.at[t - 1, :, two],
            [
                (b_h.at[t - 1, g, 2], b_h.at[t - 1, g, j], term_sem.at[k_sem + t // 2], (s, p))
                for g in both
                for j, p in sides
            ],
        )
        for t in range(1, top, 2)
    }
    w_host = Group(w_h.at[0, two], [(w_h.at[0, 2], w_h.at[0, j], op_sem.at[w_sem], (s, p)) for j, p in sides])

    def back(buf, dst, recv, t):
        return Group(
            buf.at[t - 1, :, middle], [(buf.at[t - 1, g, middle], dst.at[g], recv, (t, q)) for g in both]
        )

    back_d = {t: back(d_h, d_home, home_sem.at[0], t) for t in range(2, slabs)}
    back_u = {t: back(u_h, u_home, home_sem.at[1], t) for t in range(2, top)}
    last_u = Group(u0_s, [(u0_s.at[g], u_home.at[g], home_sem.at[1 + g], (0, q)) for g in both])
    most = max(most, names.count)
    assert most == send_sem.shape[0], most

    count = margin_ref[0, 0]
    row = lax.broadcasted_iota(jnp.int32, (KMAX, KMAX), 0)
    col = lax.broadcasted_iota(jnp.int32, (KMAX, KMAX), 1)
    hit = (row == KMAX - count + col) & (col < count)
    place[...] = jnp.where(hit, 1.0, 0.0).astype(BF)

    r_load.wait()
    for c in l_loads:
        c.wait()
    for c in map_loads:
        c.start()
    half = halfway(r_v[...].astype(BF), fac, m)
    at_tail = nn(half[:, m - KMAX :], fac[m - KMAX :, m - KMAX :]).astype(BF)
    tail_s[...] = nn(at_tail, place[...]).astype(BF)
    head_s[...] = nn(half, fac[:, :KMAX]).astype(BF)

    pl.semaphore_wait(barrier, greeted)

    def send_tails():
        start(*tail_c)

    @pl.when(first_slab)
    def _():
        tail_c[0].start()

    low = fac[:, :face]
    high = fac[m - face :, m - face :]
    k_tail = jnp.concatenate(
        [tn(low[m - KMAX :], fac[m - KMAX :, m - KMAX :]), tn(high, fac[m - face :, m - KMAX :])], axis=0
    )
    k_head = jnp.concatenate([tn(low, fac[:, :KMAX]), tn(high, fac[m - face :, :KMAX])], axis=0)
    zt_s[...] = nn(k_tail.astype(BF), place[...]).astype(BF)
    zh_s[...] = k_head.astype(BF)

    @pl.when(first_slab)
    def _():
        tail_c[1].start()

    far_right, far_left = q == patches - 1, q == 0

    def lift_far():
        @pl.when(far_right)
        def _():
            zu_c.start(0, 1)

        @pl.when(far_left)
        def _():
            zu_c.start(1, 2)

    def lift():
        @pl.when(~far_right)
        def _():
            zu_c.start(0, 1)

        @pl.when(~far_left)
        def _():
            zu_c.start(1, 2)

    @pl.when(inner_low)
    def _():
        start(zd_c)

    pl.when(guest & inner_high)(lift_far)

    arrived(maps, load_sem.at[0])
    for k, piece in enumerate(solve(maps[...], fac, m)):
        gt[:, k * KMAX : (k + 1) * KMAX] = piece.astype(BF)

    @pl.when(guest)
    def _():
        zd_c.sent()
        send_tails()

    @pl.when(first_slab)
    def _():
        tail_c[0].sent()
        pl.semaphore_signal(turn_sem, inc=1, device_id=(HOST, q), device_id_type=MESH)

    @pl.when(host)
    def _():
        pl.semaphore_wait(turn_sem, 1)
        send_tails()

    @pl.when(inner_low)
    def _():
        arrived(z_r.at[:, low_rows], near_sem.at[halves])
        zr[low_rows] = nt(z_r[1, low_rows], place[...]).astype(BF)
        own = (-gt[:, :face].astype(F32)).T.astype(BF)
        from_left = (0.5 * nt(z_r[0, low_rows], gt[:, :KMAX])).astype(BF)
        from_right = (0.5 * nt(zr[low_rows], gt[:, m - KMAX :])).astype(BF)
        for n, block in enumerate((own, from_left, from_right)):
            lines = pl.ds(n * face, face)
            t_h[below, lines] = block[:, :face]

            @pl.when(inner_high)
            def _():
                v_h[below, lines] = block[:, face:]

            @pl.when(~inner_high)
            def _():
                w_h[below, 2, lines] = block[:, face:]

        @pl.when(guest & inner_high)
        def _():
            start(t_c, v_c)

        @pl.when(last)
        def _():
            start(w_c)

    for g, w in enumerate(part):
        arrived(side_r.at[:, w], near_sem.at[g])
        adj[w, :] = r_v[w, :]
        adj[w, :KMAX] = adj[w, :KMAX] - 0.5 * side_r[0, w].astype(F32)
        adj[w, m - KMAX :] = adj[w, m - KMAX :] - 0.5 * nt(side_r[1, w], place[...])

        @pl.when(first_slab)
        def _():
            d_s[w] = nt(adj[w, :].astype(BF), gt[:face]).astype(BF)
            seed_c.start(3 * g, 3 * g + 3)

        @pl.when(inner_low)
        def _():
            terms = nt(adj[w, :].astype(BF), gt[...]).astype(BF)
            a_h[below, g] = terms[:, :face]
            b_h[below, g, 2] = terms[:, face:]

            @pl.when(guest & inner_high)
            def _():
                a_c.start(g, g + 1)
                if g == 0:
                    lift()

            @pl.when(guest)
            def _():
                b_c.start(g, g + 1)

            @pl.when(last)
            def _():
                b_swap.start(2 * g, 2 * g + 2)
                if g == 0:
                    start(w_near)

    @pl.when(last)
    def _():
        arrived(b_h.at[below, :, two], near_sem.at[halves + 2])
        start(b_pass)

    @pl.when(first_slab)
    def _():
        start(lent_c)
        for k, piece in enumerate(solve(adj[...].astype(BF), fac, m)):
            out_ref[0, 0, :, k * KMAX : (k + 1) * KMAX] = piece
        effect[:face] = (-tn(fac[m - face :, m - face :], fac[m - face :, :])).astype(BF)

    def make_up():
        arrived(z_r.at[:, high_rows], near_sem.at[halves + 1])
        zr[high_rows] = nt(z_r[1, high_rows], place[...]).astype(BF)

        @pl.when(inner_low)
        def _():
            w_h[below, 2, :face] = (-gt[face:, m - face :].astype(F32)).T.astype(BF)
            w_h[below, 2, face : 2 * face] = (0.5 * nt(z_r[0, high_rows], gt[face:, :KMAX])).astype(BF)
            w_h[below, 2, 2 * face :] = (0.5 * nt(zr[high_rows], gt[face:, m - KMAX :])).astype(BF)

    @pl.when(guest & inner_high)
    def _():
        make_up()
        start(w_c)

        @pl.when(odd)
        def _():
            start(w_near)

    @pl.when(aide)
    def _():
        arrived(lent.at[two], aide_sem.at[0])
        start(lent_near)

        @pl.when(q == 0)
        def _():
            arrived(lent.at[3], aide_sem.at[2])
            lent_back.start(1, 2)
            arrived(lent.at[2], aide_sem.at[1])
            lent_back.start(0, 1)

        @pl.when(q > 0)
        def _():
            arrived(lent.at[2], aide_sem.at[1])
            lent_back.start(0, 1)
            arrived(lent.at[3], aide_sem.at[2])
            lent_back.start(1, 2)

    def beside(ref, n, g, slots):
        return jnp.concatenate([ref[n, g, j] for j in slots], axis=1)

    centre = (OWN, LEFT, RIGHT)

    def drop_low(get):
        for g, w in enumerate(part):
            adj[w, :face] = adj[w, :face] - get(g, 2).astype(F32)
            adj[w, :KMAX] = adj[w, :KMAX] + 0.5 * nn(get(g, 0), z_r[0, low_rows])
            adj[w, m - KMAX :] = adj[w, m - KMAX :] + 0.5 * nn(get(g, 1), zr[low_rows])

    def drop_high(g, get):
        w = part[g]
        adj[w, m - face :] = adj[w, m - face :] - get(g, 2).astype(F32)
        adj[w, :KMAX] = adj[w, :KMAX] + 0.5 * nn(get(g, 0), z_r[0, high_rows])
        adj[w, m - KMAX :] = adj[w, m - KMAX :] + 0.5 * nn(get(g, 1), zr[high_rows])

    @pl.when(host)
    def _():
        for t in range(1, top):
            n = t - 1
            if t > HOST:
                arrived(t_h.at[n], op_sem.at[t_sem + n - 1])
            for g in both:
                if t > HOST:
                    arrived(a_h.at[n, g], term_sem.at[a_sem + halves * (n - 1) + g])
                arrived(d_h.at[n, g, pl.ds(2, 3 if t == 1 else 2)], ring_sem.at[ring_of(0, t) + g])
                d_h[n + 1, g, OWN] = (a_h[n, g].astype(F32) + nn(beside(d_h, n, g, centre), t_h[n])).astype(BF)
                per = len(far if t + 1 == top else close)
                round_d[t + 1].start(per * g, per * g + per)
            if t == 1:
                start(zu_c)
            if t > HOST:
                back_d[t].start()
                if t % 2 == 0:
                    kept_c[t - 1].start()
                arrived(v_h.at[n], op_sem.at[v_sem + n - 1])
                arrived(b_h.at[n, :, 2], term_sem.at[b_sem + n - 1])
            for g in both:
                b_h[n, g, 2] = (b_h[n, g, 2].astype(F32) + nn(beside(d_h, n, g, centre), v_h[n])).astype(BF)
            if t == min(2, top - 1):
                make_up()
                start(w_host)

        drop_low(lambda g, j: d_h[0, g, 2 + j])
        arrived(w_h.at[top - 1], op_sem.at[w_sem + top - 1])
        for t in range(top, 0, -2):
            n = t - 1
            state = d_h if t == top else u_h
            if t < top:
                arrived(w_h.at[n, two] if t == HOST else w_h.at[n], op_sem.at[w_sem + n])
            if t > 1:
                arrived(w_h.at[n - 1, 2], op_sem.at[w_sem + n - 1])
            if t == top:
                arrived(b_h.at[n], term_sem.at[b_sem + n - 1])
            else:
                arrived(b_h.at[n, :, two], term_sem.at[k_sem + t // 2])
            for g in both:
                arrived(state.at[n, g, four], ring_sem.at[ring_of(0 if t == top else 1, t) + g])
                for j, slots in enumerate(((LEFT, FAR_LEFT, OWN), (RIGHT, OWN, FAR_RIGHT), centre)):
                    u = (b_h[n, g, j].astype(F32) + nn(beside(state, n, g, slots), w_h[n, j])).astype(BF)
                    if t > 1:
                        u_h[n - 1, g, 2 + j] = u
                    else:
                        u0_s[g, j] = u
                if t > 1:
                    u = b_h[n - 1, g, 2].astype(F32) + nn(beside(u_h, n - 1, g, centre), w_h[n - 1, 2])
                    u_h[n - 2, g, OWN] = u.astype(BF)
                    round_u[t - 2].start(4 * g, 4 * g + 4)
                    back_u[t - 1].start(g, g + 1)
                else:
                    last_u.start(g, g + 1)
                if t > HOST:
                    (back_d if t == top else back_u)[t].start(g, g + 1)

    @pl.when(host)
    def _():
        if HOST < top:
            for g in both:
                drop_high(g, lambda g, j: u_h[0, g, 2 + j])

    @pl.when(guest)
    def _():
        arrived(d_home, home_sem.at[0])
        drop_low(lambda g, j: d_home[g, j])

    @pl.when(guest & inner_high)
    def _():
        arrived(u_home, home_sem.at[1])
        for g in both:
            drop_high(g, lambda g, j: u_home[g, j])

    @pl.when(first_slab)
    def _():
        arrived(z_r.at[:, high_rows], near_sem.at[halves + 1])
        half = jnp.concatenate(
            [nt(z_r[0, high_rows], fac[i : i + KMAX, :KMAX]).astype(BF) for i in range(0, m, KMAX)], axis=1
        )
        for k in range(0, m, KMAX):
            spread = 0.5 * nn(half[:, k:], fac[k:, k : k + KMAX])
            effect[face : 2 * face, k : k + KMAX] = spread.astype(BF)
        at_tail = nt(z_r[1, high_rows], place[...]).astype(BF)
        half = nt(at_tail, fac[m - KMAX :, m - KMAX :]).astype(BF)
        effect[2 * face :] = (0.5 * nn(half, fac[m - KMAX :, :])).astype(BF)
        for g, w in enumerate(part):
            arrived(u_home.at[g], home_sem.at[1 + g])
            u = jnp.concatenate([u_home[g, j] for j in (2, 0, 1)], axis=1)
            out_ref[0, 0, w, :] = out_ref[0, 0, w, :] + nn(u, effect[...])

    @pl.when(inner_low)
    def _():
        for k, piece in enumerate(solve(adj[...].astype(BF), fac, m)):
            out_ref[0, 0, :, k * KMAX : (k + 1) * KMAX] = piece

    @pl.when(first_slab)
    def _():
        sent(tail_c[1], lent_c, seed_c)

    @pl.when(inner_low)
    def _():
        sent(tail_c[1])

    @pl.when(host)
    def _():
        sent(zd_c, tail_c[0])

    @pl.when(guest)
    def _():
        sent(tail_c[0])

    @pl.when(inner_low & inner_high)
    def _():
        sent(zu_c)

    @pl.when(aide)
    def _():
        sent(lent_near, lent_back)

    @pl.when(guest)
    def _():
        sent(w_c, b_c)

    @pl.when(guest & inner_high)
    def _():
        sent(t_c, v_c, a_c)

    @pl.when(odd_guest)
    def _():
        sent(w_near)

    @pl.when(last)
    def _():
        sent(b_swap, b_pass)

    @pl.when(host)
    def _():
        sent(w_host, last_u)
        for kind in (round_d, round_u, kept_c, back_d, back_u):
            sent(*kind.values())


def on_device(slabs, patches, right_side, inverse_factor, forward_trace, backward_trace, margin):
    cols, m = right_side.shape[2:]
    face = forward_trace.shape[2]
    halves = 2
    rows = cols // halves
    links = slabs - 1
    wide = pltpu.VMEM((cols, KMAX), BF)
    square = pltpu.VMEM((2 * face, KMAX), BF)
    hbm = pl.BlockSpec(memory_space=pltpu.HBM)
    home = pltpu.VMEM((halves, 3, rows, face), BF)
    ops = pltpu.VMEM((links, 3 * face, face), BF)
    ring = pltpu.VMEM((links, halves, 5, rows, face), BF)
    sends = halves + 2 + max(10, 2 * (links - 1) + (links - 2) + 3 * (slabs // 2 - 1) - (slabs // 2 - 1) + 2)
    return pl.pallas_call(
        functools.partial(kernel, slabs, patches, halves),
        out_shape=pltpu.VMEM(right_side.shape, F32),
        in_specs=[hbm, hbm, hbm, hbm, pl.BlockSpec(memory_space=pltpu.SMEM)],
        out_specs=pl.BlockSpec(memory_space=pltpu.VMEM),
        scratch_shapes=[
            pltpu.VMEM((cols, m), F32),
            pltpu.VMEM((m, m), BF),
            pltpu.VMEM((2 * face, m), BF),
            wide, wide, square, square, pltpu.VMEM((cols, face), BF),
            pltpu.VMEM((2, cols, KMAX), BF), pltpu.VMEM((2, 2 * face, KMAX), BF), home, home,
            pltpu.VMEM((links, halves, rows, face), BF),
            pltpu.VMEM((links, halves, 3, rows, face), BF),
            ops, ops, pltpu.VMEM((links, 3, 3 * face, face), BF),
            ring, ring, home,
            pltpu.VMEM((cols, m), F32),
            pltpu.VMEM((2 * face, m), BF),
            pltpu.VMEM((KMAX, KMAX), BF),
            square,
            pltpu.VMEM((4, face, KMAX), BF),
            pltpu.VMEM((3 * face, m), BF),
            pltpu.SemaphoreType.DMA((2 + m // KMAX,)),
            pltpu.SemaphoreType.DMA((sends,)),
            pltpu.SemaphoreType.DMA((halves + 3,)),
            pltpu.SemaphoreType.DMA((1 + halves,)),
            pltpu.SemaphoreType.DMA((2 * (links - 2) + links,)),
            pltpu.SemaphoreType.DMA((halves * (links - 2) + links - 1 + slabs // 2 - 1,)),
            pltpu.SemaphoreType.DMA((halves * (links + slabs // 2 - 1),)),
            pltpu.SemaphoreType.DMA((3,)),
            pltpu.SemaphoreType.REGULAR,
        ],
        compiler_params=pltpu.CompilerParams(collective_id=0, has_side_effects=True),
        name="sweeps",
    )(right_side, inverse_factor, forward_trace, backward_trace, margin)
    return pl.pallas_call(
        finish,
        out_shape=jax.ShapeDtypeStruct(right_side.shape, F32),
        in_specs=[pl.BlockSpec(memory_space=pltpu.VMEM)] * 2,
        out_specs=hbm,
        scratch_shapes=[pltpu.VMEM((m // KMAX, cols, KMAX), F32), pltpu.SemaphoreType.DMA((m // KMAX,))],
        compiler_params=pltpu.CompilerParams(vmem_limit_bytes=16 << 20),
        name="finish",
    )(half, inverse_factor)


def solution(mesh):
    four = P("slab", "patch", None, None)
    return jax.shard_map(
        functools.partial(on_device, mesh.shape["slab"], mesh.shape["patch"]),
        mesh=mesh,
        in_specs=(four, four, four, four, P("slab", "patch")),
        out_specs=four,
        check_vma=False,
    )
```
